256 devices in a mesh: batch: 4 (over x_lo, core), seq: 64 (over y, x_hi, z).
Axes of the slice: x: 4 (x_hi: 2, x_lo: 2; x = x_hi * 2 + x_lo), y: 4, z: 8, core: 2. Of those that a mesh axis runs over, the one named last changes fastest.
Arguments:
- signal: bfloat16 [4, 16384, 256], P('batch', 'seq'), may hold values from -0.125 to 0.125
- grad_out: bfloat16 [4, 16384, 256], P('batch', 'seq'), may hold values from -6 to 6
- filter_taps: float32 [16384, 256], P('seq'), may hold values from -0.125 to 0.125
- skip_gain: float32 [256], replicated, may hold values from 0.5 to 2
Outputs:
- input_grad: bfloat16 [4, 16384, 256], P('batch', 'seq')
- filter_grad: float32 [16384, 256], P('seq')
The draws below stay inside these ranges and needn't reach their ends.
All inputs are finite; a program needn't handle non-finite values.
Results may differ from the reference program's by a relative error of at most 0.001.
Values sent between devices are 32-bit elements; how exact they have to be, the bound alone decides.
A program may use at most 64 MiB of HBM per device.

```python
import jax
import jax.numpy as jnp

CHANNELS = 256
LENGTH = 16384
BATCH = 4


def levels(stream_key, dims, pieces, least, high):
    factor_of, own = 1.0, jax.random.fold_in(stream_key, 6)
    for dim, blocks in pieces:
        heights = jnp.exp(jax.random.uniform(jax.random.fold_in(own, dim), (blocks,), jnp.float32, least / len(pieces), high / len(pieces)))
        factor_of = factor_of * jnp.repeat(heights, dims[dim] // blocks).reshape([-1 if axis == dim else 1 for axis in range(len(dims))])
    return factor_of


def scatter_about(own_key, dims, width, bound, shards=(), dtype=jnp.bfloat16):
    array = width * jax.random.normal(own_key, dims, jnp.float32)
    if shards:
        array = array * levels(own_key, dims, shards, -0.22, 0.18)
    return jnp.clip(array, -bound, bound).astype(dtype)


def setup_inputs(seed: int = 0) -> dict:
    keys = jax.random.split(jax.random.key(seed), 5)
    return {
        "signal": scatter_about(keys[0], (BATCH, LENGTH, CHANNELS), (LENGTH ** -0.5), 0.125, ((0, 4), (1, 64))),
        "grad_out": scatter_about(keys[1], (BATCH, LENGTH, CHANNELS), 1.0, 6.0, ((0, 4), (1, 64))),
        "filter_taps": scatter_about(keys[2], (LENGTH, CHANNELS), (LENGTH ** -0.5), 0.125, ((0, 64),), jnp.float32),
        "skip_gain": jnp.clip(jax.random.uniform(keys[3], (CHANNELS,), jnp.float32, 0.5, 2.0), 0.5, 2.0),
    }


def reference(signal, grad_out, filter_taps, skip_gain):
    length = signal.shape[1]
    padded_len = 2 * length
    signal_full = signal.astype(jnp.float32)
    grad_full = grad_out.astype(jnp.float32)
    signal_spec = jnp.fft.rfft(signal_full, n=padded_len, axis=1)
    grad_spec = jnp.fft.rfft(grad_full, n=padded_len, axis=1)
    taps_spec = jnp.fft.rfft(filter_taps, n=padded_len, axis=0)
    input_conv = jnp.fft.irfft(grad_spec * jnp.conj(taps_spec)[None], n=padded_len, axis=1)[:, :length]
    input_grad = (input_conv + skip_gain[None, None, :] * grad_full).astype(jnp.bfloat16)
    summed = jnp.sum(grad_spec * jnp.conj(signal_spec), axis=0)
    filter_grad = jnp.fft.irfft(summed, n=padded_len, axis=0)[:length]
    return input_grad, filter_grad.astype(jnp.float32)
```

```python
import ml_dtypes
import numpy as np
import jax
import jax.numpy as jnp
from jax import lax
from jax.experimental import pallas as pl
from jax.experimental.pallas import tpu as pltpu
from jax.sharding import PartitionSpec as P


F32 = jnp.float32
BF16 = jnp.bfloat16
SIDE = 128
LEN = SIDE * SIDE
MESH = pl.DeviceIdType.MESH
TAPS, GRAD, SIGNAL, INPUT, FILTER, SWAP_GRAD, SWAP_SIGNAL, SWAP_INPUT, SWAP_FILTER = range(9)


def split_table(table):
    high = table.astype(np.float32).astype(ml_dtypes.bfloat16)
    low = (table - high.astype(np.float64)).astype(np.float32).astype(ml_dtypes.bfloat16)
    return high, low


def tables():
    index = np.arange(SIDE)
    angle = 2 * np.pi * (np.outer(4 * index + 1, index) % (4 * SIDE)) / (4.0 * SIDE)
    high, low = split_table(np.concatenate([np.cos(angle), -np.sin(angle)], axis=0))
    first = np.concatenate([high, low, high], axis=1)
    fine = 2 * np.pi * (np.outer(index, index) % SIDE) / float(SIDE)
    cos_fine, sin_fine = np.cos(fine), np.sin(fine)
    second = np.stack(split_table(np.block([[cos_fine, -sin_fine], [sin_fine, cos_fine]])))
    third = np.stack(split_table(np.block([[cos_fine, sin_fine], [-sin_fine, cos_fine]])))
    fourth = np.stack(split_table(np.concatenate([np.cos(angle.T), -np.sin(angle.T)], axis=1) / LEN))
    turn = 2 * np.pi * np.outer(4 * index + 1, index) / (4.0 * LEN)
    turns = np.stack([np.cos(turn), np.sin(turn)]).astype(np.float32)
    return tuple(jnp.asarray(table) for table in (first, second, third, fourth, turns))


def split(value):
    high = value.astype(BF16)
    return high, (value - high.astype(F32)).astype(BF16)


def dot(left, right):
    return jnp.dot(left, right, preferred_element_type=F32)


def body(
    signal, grad, taps, gain, first, second, third, fourth, turns,
    out_input, out_filter,
    send_taps, send_grad, send_signal, stage_grad, stage_signal, land_taps, land_grad, land_signal,
    send_input, send_filter, land_input, land_filter, pair_input, pair_filter,
    coarse, rows_high, rows_low, spectra, columns_high, columns_low,
    sends, recvs,
):
    batch = lax.axis_index("batch")
    seq = lax.axis_index("seq")
    core = batch % 2
    x_low = batch // 2
    x_pos = 2 * ((seq // 8) % 2) + x_low
    y_pos = seq // 16
    z_pos = seq % 8
    me = x_low * 64 + seq
    partner = (batch + 1 - 2 * core, seq)
    own = pl.multiple_of(core * SIDE, SIDE)
    other = pl.multiple_of((1 - core) * SIDE, SIDE)

    def each_peer(act):
        for dz in (4, 3, 5, 2, 6, 1, 7, 0):

            def one(step, carry, dz=dz):
                x_to = (x_pos + step % 4) % 4
                y_to = (y_pos + step // 4) % 4
                z_to = (z_pos + dz * (1 - 2 * core) + 8) % 8
                act(x_to % 2, y_to * 16 + (x_to // 2) * 8 + z_to)
                return carry

            lax.fori_loop(1 if dz == 0 else 0, 16, one, 0)

    def copy(source, landing, slot, device):
        return pltpu.make_async_remote_copy(
            src_ref=source, dst_ref=landing, send_sem=sends.at[slot], recv_sem=recvs.at[slot],
            device_id=device, device_id_type=MESH,
        )

    def send_all(source_of, landing, slot):
        each_peer(
            lambda x, s: copy(source_of(x, s), landing, slot, (2 * x + core, s)).start()
        )

    barrier = pltpu.get_barrier_semaphore()
    each_peer(
        lambda x, s: pl.semaphore_signal(
            barrier, inc=1, device_id=(2 * x + core, s), device_id_type=MESH
        )
    )
    pl.semaphore_signal(barrier, inc=1, device_id=partner, device_id_type=MESH)

    for array, stage, send in ((grad, stage_grad, send_grad), (signal, stage_signal, send_signal)):
        for half in range(2):
            rows = pl.ds(half * SIDE, SIDE)
            spread = pl.ds(half, SIDE, stride=2)
            stage[spread, :] = array[rows, pl.ds(other, SIDE)].astype(F32).T
            send[core, spread, :] = array[rows, pl.ds(own, SIDE)].astype(F32).T
    send_taps[...] = taps[pl.ds(pl.multiple_of(x_low * SIDE, SIDE), SIDE), pl.ds(own, SIDE)].T
    pl.semaphore_wait(barrier, 128)

    swap_grad = copy(stage_grad, send_grad.at[core], SWAP_GRAD, partner)
    swap_signal = copy(stage_signal, send_signal.at[core], SWAP_SIGNAL, partner)
    swap_grad.start()
    swap_signal.start()

    taps_at = land_taps.at[pl.ds(2 * seq + x_low, 1)]
    send_all(lambda x, s: send_taps.at[pl.ds(64 * x + s, 1)], taps_at, TAPS)
    land_taps[pl.ds(2 * seq + x_low, 1), :] = send_taps[pl.ds(me, 1), :]

    for swap, send, land, slot in (
        (swap_grad, send_grad, land_grad, GRAD),
        (swap_signal, send_signal, land_signal, SIGNAL),
    ):
        swap.wait()
        send_all(
            lambda x, s, send=send: send.at[:, pl.ds(2 * (64 * x + s), 2), :],
            land.at[pl.ds(2 * x_low, 2), pl.ds(2 * seq, 2), :],
            slot,
        )
        for b in range(2):
            land[2 * x_low + b, pl.ds(2 * seq, 2), :] = send[b, pl.ds(2 * me, 2), :]

    all_taps = copy(land_taps.at[pl.ds(0, 127)], land_taps.at[pl.ds(0, 127)], TAPS, partner)
    all_grad, all_signal = (
        copy(land.at[:, pl.ds(0, 127), :], land.at[:, pl.ds(0, 127), :], slot, partner)
        for land, slot in ((land_grad, GRAD), (land_signal, SIGNAL))
    )

    cos_turn, sin_turn = turns[0], turns[1]

    def turn_forward(count):
        for b in range(count):
            real = coarse[:SIDE, b * SIDE : (b + 1) * SIDE]
            imag = coarse[SIDE:, b * SIDE : (b + 1) * SIDE]
            rows = pl.ds(b * SIDE, SIDE)
            rows_high[rows, :SIDE], rows_low[rows, :SIDE] = split(real * cos_turn + imag * sin_turn)
            rows_high[rows, SIDE:], rows_low[rows, SIDE:] = split(imag * cos_turn - real * sin_turn)

    def along_rows(table, count):
        rows = pl.ds(0, count * SIDE)
        return (
            dot(rows_high[rows, :], table[0])
            + dot(rows_low[rows, :], table[0])
            + dot(rows_high[rows, :], table[1])
        )

    def exact_columns(land):
        columns = jnp.concatenate([land[b].astype(BF16) for b in range(4)], axis=1)
        return dot(first[:, : 2 * SIDE], jnp.concatenate([columns, columns], axis=0))

    def inverse(products, count):
        for b in range(count):
            real, imag = products[b]
            rows = pl.ds(b * SIDE, SIDE)
            rows_high[rows, :SIDE], rows_low[rows, :SIDE] = split(real)
            rows_high[rows, SIDE:], rows_low[rows, SIDE:] = split(imag)
        lines = along_rows(third, count)
        for b in range(count):
            real = lines[b * SIDE : (b + 1) * SIDE, :SIDE]
            imag = lines[b * SIDE : (b + 1) * SIDE, SIDE:]
            where = pl.ds(b * SIDE, SIDE)
            columns_high[:SIDE, where], columns_low[:SIDE, where] = split(real * cos_turn - imag * sin_turn)
            columns_high[SIDE:, where], columns_low[SIDE:, where] = split(real * sin_turn + imag * cos_turn)
        where = pl.ds(0, count * SIDE)
        return (
            dot(fourth[0], columns_high[:, where])
            + dot(fourth[0], columns_low[:, where])
            + dot(fourth[1], columns_high[:, where])
        )

    def times_conjugate(left, right):
        return (
            left[0] * right[0] + left[1] * right[1],
            left[1] * right[0] - left[0] * right[1],
        )

    def spectrum(b):
        rows = pl.ds(b * SIDE, SIDE)
        return spectra[rows, :SIDE], spectra[rows, SIDE:]

    all_taps.wait()
    taps_high, taps_low = split(land_taps[...])
    coarse[:, 4 * SIDE :] = dot(first[...], jnp.concatenate([taps_high, taps_high, taps_low], axis=0))
    all_grad.wait()
    coarse[:, : 4 * SIDE] = exact_columns(land_grad)
    turn_forward(5)
    spectra[...] = along_rows(second, 5)
    filter_spectrum = spectrum(4)
    values = inverse([times_conjugate(spectrum(b), filter_spectrum) for b in range(4)], 4)
    for b in range(4):
        send_input[b] = values[:, b * SIDE : (b + 1) * SIDE]
    send_all(
        lambda x, s: send_input.at[pl.ds(2 * x, 2), pl.ds(2 * s, 2), :],
        land_input.at[:, pl.ds(2 * me, 2), :],
        INPUT,
    )
    for b in range(2):
        land_input[b, pl.ds(2 * me, 2), :] = send_input[2 * x_low + b, pl.ds(2 * seq, 2), :]

    all_signal.wait()
    coarse[:, : 4 * SIDE] = exact_columns(land_signal)
    turn_forward(4)
    signal_spectra = along_rows(second, 4)
    total_real, total_imag = 0.0, 0.0
    for b in range(4):
        lines = signal_spectra[b * SIDE : (b + 1) * SIDE]
        real, imag = times_conjugate(spectrum(b), (lines[:, :SIDE], lines[:, SIDE:]))
        total_real, total_imag = total_real + real, total_imag + imag
    send_filter[...] = inverse([(total_real, total_imag)], 1)
    send_all(
        lambda x, s: send_filter.at[pl.ds(2 * s, 2), :], land_filter.at[pl.ds(2 * me, 2), :], FILTER
    )
    land_filter[pl.ds(2 * me, 2), :] = send_filter[pl.ds(2 * seq, 2), :]

    all_input = copy(land_input.at[:, pl.ds(0, 254), :], land_input.at[:, pl.ds(0, 254), :], INPUT, partner)
    all_input.wait()
    swap_input = copy(land_input.at[1 - core], pair_input, SWAP_INPUT, partner)
    swap_input.start()

    def finish_input(block_of, lanes):
        for half in range(2):
            rows = pl.ds(half * SIDE, SIDE)
            skip = gain[:, pl.ds(lanes, SIDE)] * grad[rows, pl.ds(lanes, SIDE)].astype(F32)
            out_input[rows, pl.ds(lanes, SIDE)] = (block_of(half).T + skip).astype(BF16)

    finish_input(lambda half: land_input[core, pl.ds(half, SIDE, stride=2), :], own)
    swap_input.wait()
    finish_input(lambda half: pair_input[pl.ds(half, SIDE, stride=2), :], other)

    all_filter = copy(land_filter.at[pl.ds(0, 254)], land_filter.at[pl.ds(0, 254)], FILTER, partner)
    all_filter.wait()
    swap_filter = copy(land_filter, pair_filter, SWAP_FILTER, partner)
    swap_filter.start()
    for half in range(2):
        out_filter[pl.ds(half * SIDE, SIDE), pl.ds(own, SIDE)] = land_filter[pl.ds(half, SIDE, stride=2), :].T
    swap_filter.wait()
    for half in range(2):
        out_filter[pl.ds(half * SIDE, SIDE), pl.ds(other, SIDE)] = pair_filter[pl.ds(half, SIDE, stride=2), :].T


def shards(signal, grad_out, filter_taps, skip_gain):
    vmem = pl.BlockSpec(memory_space=pltpu.VMEM)
    rows = lambda *shape: pltpu.VMEM((*shape, SIDE), F32)
    input_grad, filter_grad = pl.pallas_call(
        body,
        out_shape=(
            jax.ShapeDtypeStruct((2 * SIDE, 2 * SIDE), BF16),
            jax.ShapeDtypeStruct((2 * SIDE, 2 * SIDE), F32),
        ),
        in_specs=[vmem] * 9,
        out_specs=(vmem, vmem),
        scratch_shapes=[
            rows(SIDE), rows(2, 2 * SIDE), rows(2, 2 * SIDE), rows(2 * SIDE), rows(2 * SIDE),
            rows(SIDE), rows(4, SIDE), rows(4, SIDE),
            rows(4, SIDE), rows(SIDE), rows(2, 2 * SIDE), rows(2 * SIDE), rows(2 * SIDE), rows(2 * SIDE),
            pltpu.VMEM((2 * SIDE, 5 * SIDE), F32),
            pltpu.VMEM((5 * SIDE, 2 * SIDE), BF16),
            pltpu.VMEM((5 * SIDE, 2 * SIDE), BF16),
            pltpu.VMEM((5 * SIDE, 2 * SIDE), F32),
            pltpu.VMEM((2 * SIDE, 4 * SIDE), BF16),
            pltpu.VMEM((2 * SIDE, 4 * SIDE), BF16),
            pltpu.SemaphoreType.DMA((9,)),
            pltpu.SemaphoreType.DMA((9,)),
        ],
        compiler_params=pltpu.CompilerParams(collective_id=0, has_side_effects=True),
    )(signal[0], grad_out[0], filter_taps, skip_gain[None, :], *tables())
    return input_grad[None], filter_grad


def solution(mesh):
    return jax.shard_map(
        shards,
        mesh=mesh,
        in_specs=(P("batch", "seq", None), P("batch", "seq", None), P("seq", None), P()),
        out_specs=(P("batch", "seq", None), P("seq", None)),
        check_vma=False,
    )
```

```python
import ml_dtypes
import numpy as np
import jax
import jax.numpy as jnp
from jax import lax
from jax.experimental import pallas as pl
from jax.experimental.pallas import tpu as pltpu
from jax.sharding import PartitionSpec as P


F32 = jnp.float32
BF16 = jnp.bfloat16
SIDE = 128
LEN = SIDE * SIDE
MESH = pl.DeviceIdType.MESH
TAPS, GRAD, SIGNAL, INPUT, FILTER, SWAP_GRAD, SWAP_SIGNAL, SWAP_INPUT, SWAP_FILTER = range(9)


def split_table(table):
    high = table.astype(np.float32).astype(ml_dtypes.bfloat16)
    low = (table - high.astype(np.float64)).astype(np.float32).astype(ml_dtypes.bfloat16)
    return high, low


def tables():
    index = np.arange(SIDE)
    angle = 2 * np.pi * (np.outer(4 * index + 1, index) % (4 * SIDE)) / (4.0 * SIDE)
    high, low = split_table(np.concatenate([np.cos(angle), -np.sin(angle)], axis=0))
    first = np.concatenate([high, low, high], axis=1)
    fine = 2 * np.pi * (np.outer(index, index) % SIDE) / float(SIDE)
    cos_fine, sin_fine = np.cos(fine), np.sin(fine)
    second = np.stack(split_table(np.block([[cos_fine, -sin_fine], [sin_fine, cos_fine]])))
    third = np.stack(split_table(np.block([[cos_fine, sin_fine], [-sin_fine, cos_fine]])))
    fourth = np.stack(split_table(np.concatenate([np.cos(angle.T), -np.sin(angle.T)], axis=1) / LEN))
    turn = 2 * np.pi * np.outer(4 * index + 1, index) / (4.0 * LEN)
    turns = np.stack([np.cos(turn), np.sin(turn)]).astype(np.float32)
    return tuple(jnp.asarray(table) for table in (first, second, third, fourth, turns))


def split(value):
    high = value.astype(BF16)
    return high, (value - high.astype(F32)).astype(BF16)


def dot(left, right):
    return jnp.dot(left, right, preferred_element_type=F32)


def body(
    signal_far, grad_far, taps_far, gain_far, *rest
):
    (
        tables_far, (out_input, out_filter), (signal, grad, taps, gain), held_tables, rest
    ) = rest[:5], rest[5:7], rest[7:11], rest[11:16], rest[16:]
    run(signal_far, grad_far, taps_far, gain_far, tables_far, out_input, out_filter,
        signal, grad, taps, gain, *held_tables, held_tables, *rest)


def run(
    signal_far, grad_far, taps_far, gain_far, tables_far,
    out_input, out_filter,
    signal, grad, taps, gain, first, second, third, fourth, turns, held_tables,
    send_taps, send_grad, send_signal, stage_grad, stage_signal, land_taps, land_grad, land_signal,
    send_input, send_filter, land_input, land_filter, pair_input, pair_filter,
    coarse, rows_high, rows_low, spectra, columns_high, columns_low,
    sends, recvs, loads,
):
    batch = lax.axis_index("batch")
    seq = lax.axis_index("seq")
    core = batch % 2
    x_low = batch // 2
    x_pos = 2 * ((seq // 8) % 2) + x_low
    y_pos = seq // 16
    z_pos = seq % 8
    me = x_low * 64 + seq
    partner = (batch + 1 - 2 * core, seq)
    own = pl.multiple_of(core * SIDE, SIDE)
    other = pl.multiple_of((1 - core) * SIDE, SIDE)

    def each_peer(act):
        for dz in (4, 3, 5, 2, 6, 1, 7, 0):

            def one(step, carry, dz=dz):
                x_to = (x_pos + step % 4) % 4
                y_to = (y_pos + step // 4) % 4
                z_to = (z_pos + dz * (1 - 2 * core) + 8) % 8
                act(x_to % 2, y_to * 16 + (x_to // 2) * 8 + z_to)
                return carry

            lax.fori_loop(1 if dz == 0 else 0, 16, one, 0)

    def copy(source, landing, slot, device):
        return pltpu.make_async_remote_copy(
            src_ref=source, dst_ref=landing, send_sem=sends.at[slot], recv_sem=recvs.at[slot],
            device_id=device, device_id_type=MESH,
        )

    def send_all(source_of, landing, slot):
        each_peer(
            lambda x, s: copy(source_of(x, s), landing, slot, (2 * x + core, s)).start()
        )

    x_rows = pl.ds(pl.multiple_of(x_low * SIDE, SIDE), SIDE)
    load_grad, load_signal, load_taps, load_gain, *load_tables = [
        pltpu.make_async_copy(far, near, loads.at[slot])
        for slot, (far, near) in enumerate(
            [
                (grad_far, grad), (signal_far, signal), (taps_far.at[x_rows, pl.ds(own, SIDE)], taps),
                (gain_far, gain), *zip(tables_far, held_tables),
            ]
        )
    ]
    for load in (load_grad, load_signal, load_taps, load_gain, *load_tables):
        load.start()

    barrier = pltpu.get_barrier_semaphore()
    each_peer(
        lambda x, s: pl.semaphore_signal(
            barrier, inc=1, device_id=(2 * x + core, s), device_id_type=MESH
        )
    )
    pl.semaphore_signal(barrier, inc=1, device_id=partner, device_id_type=MESH)

    for load, array, stage, send in (
        (load_grad, grad, stage_grad, send_grad), (load_signal, signal, stage_signal, send_signal)
    ):
        load.wait()
        for half in range(2):
            rows = pl.ds(half * SIDE, SIDE)
            spread = pl.ds(half, SIDE, stride=2)
            stage[spread, :] = array[rows, pl.ds(other, SIDE)].astype(F32).T
            send[core, spread, :] = array[rows, pl.ds(own, SIDE)].astype(F32).T
    load_taps.wait()
    send_taps[...] = taps[...].T
    pl.semaphore_wait(barrier, 128)

    swap_grad = copy(stage_grad, send_grad.at[core], SWAP_GRAD, partner)
    swap_signal = copy(stage_signal, send_signal.at[core], SWAP_SIGNAL, partner)
    swap_grad.start()
    swap_signal.start()

    taps_at = land_taps.at[pl.ds(2 * seq + x_low, 1)]
    send_all(lambda x, s: send_taps.at[pl.ds(64 * x + s, 1)], taps_at, TAPS)
    land_taps[pl.ds(2 * seq + x_low, 1), :] = send_taps[pl.ds(me, 1), :]

    for swap, send, land, slot in (
        (swap_grad, send_grad, land_grad, GRAD),
        (swap_signal, send_signal, land_signal, SIGNAL),
    ):
        swap.wait()
        send_all(
            lambda x, s, send=send: send.at[:, pl.ds(2 * (64 * x + s), 2), :],
            land.at[pl.ds(2 * x_low, 2), pl.ds(2 * seq, 2), :],
            slot,
        )
        for b in range(2):
            land[2 * x_low + b, pl.ds(2 * seq, 2), :] = send[b, pl.ds(2 * me, 2), :]

    all_taps = copy(land_taps.at[pl.ds(0, 127)], land_taps.at[pl.ds(0, 127)], TAPS, partner)
    all_grad, all_signal = (
        copy(land.at[:, pl.ds(0, 127), :], land.at[:, pl.ds(0, 127), :], slot, partner)
        for land, slot in ((land_grad, GRAD), (land_signal, SIGNAL))
    )

    for load in (load_gain, *load_tables):
        load.wait()
    cos_turn, sin_turn = turns[0], turns[1]

    def turn_forward(count):
        for b in range(count):
            real = coarse[:SIDE, b * SIDE : (b + 1) * SIDE]
            imag = coarse[SIDE:, b * SIDE : (b + 1) * SIDE]
            rows = pl.ds(b * SIDE, SIDE)
            rows_high[rows, :SIDE], rows_low[rows, :SIDE] = split(real * cos_turn + imag * sin_turn)
            rows_high[rows, SIDE:], rows_low[rows, SIDE:] = split(imag * cos_turn - real * sin_turn)

    def along_rows(table, count):
        rows = pl.ds(0, count * SIDE)
        return (
            dot(rows_high[rows, :], table[0])
            + dot(rows_low[rows, :], table[0])
            + dot(rows_high[rows, :], table[1])
        )

    def exact_columns(land):
        columns = jnp.concatenate([land[b].astype(BF16) for b in range(4)], axis=1)
        return dot(first[:, : 2 * SIDE], jnp.concatenate([columns, columns], axis=0))

    def inverse(products, count):
        for b in range(count):
            real, imag = products[b]
            rows = pl.ds(b * SIDE, SIDE)
            rows_high[rows, :SIDE], rows_low[rows, :SIDE] = split(real)
            rows_high[rows, SIDE:], rows_low[rows, SIDE:] = split(imag)
        lines = along_rows(third, count)
        for b in range(count):
            real = lines[b * SIDE : (b + 1) * SIDE, :SIDE]
            imag = lines[b * SIDE : (b + 1) * SIDE, SIDE:]
            where = pl.ds(b * SIDE, SIDE)
            columns_high[:SIDE, where], columns_low[:SIDE, where] = split(real * cos_turn - imag * sin_turn)
            columns_high[SIDE:, where], columns_low[SIDE:, where] = split(real * sin_turn + imag * cos_turn)
        where = pl.ds(0, count * SIDE)
        return (
            dot(fourth[0], columns_high[:, where])
            + dot(fourth[0], columns_low[:, where])
            + dot(fourth[1], columns_high[:, where])
        )

    def times_conjugate(left, right):
        return (
            left[0] * right[0] + left[1] * right[1],
            left[1] * right[0] - left[0] * right[1],
        )

    def spectrum(b):
        rows = pl.ds(b * SIDE, SIDE)
        return spectra[rows, :SIDE], spectra[rows, SIDE:]

    all_taps.wait()
    taps_high, taps_low = split(land_taps[...])
    coarse[:, 4 * SIDE :] = dot(first[...], jnp.concatenate([taps_high, taps_high, taps_low], axis=0))
    all_grad.wait()
    coarse[:, : 4 * SIDE] = exact_columns(land_grad)
    turn_forward(5)
    spectra[...] = along_rows(second, 5)
    filter_spectrum = spectrum(4)
    values = inverse([times_conjugate(spectrum(b), filter_spectrum) for b in range(4)], 4)
    for b in range(4):
        send_input[b] = values[:, b * SIDE : (b + 1) * SIDE]
    send_all(
        lambda x, s: send_input.at[pl.ds(2 * x, 2), pl.ds(2 * s, 2), :],
        land_input.at[:, pl.ds(2 * me, 2), :],
        INPUT,
    )
    for b in range(2):
        land_input[b, pl.ds(2 * me, 2), :] = send_input[2 * x_low + b, pl.ds(2 * seq, 2), :]

    all_signal.wait()
    coarse[:, : 4 * SIDE] = exact_columns(land_signal)
    turn_forward(4)
    signal_spectra = along_rows(second, 4)
    total_real, total_imag = 0.0, 0.0
    for b in range(4):
        lines = signal_spectra[b * SIDE : (b + 1) * SIDE]
        real, imag = times_conjugate(spectrum(b), (lines[:, :SIDE], lines[:, SIDE:]))
        total_real, total_imag = total_real + real, total_imag + imag
    send_filter[...] = inverse([(total_real, total_imag)], 1)
    send_all(
        lambda x, s: send_filter.at[pl.ds(2 * s, 2), :], land_filter.at[pl.ds(2 * me, 2), :], FILTER
    )
    land_filter[pl.ds(2 * me, 2), :] = send_filter[pl.ds(2 * seq, 2), :]

    all_input = copy(land_input.at[:, pl.ds(0, 254), :], land_input.at[:, pl.ds(0, 254), :], INPUT, partner)
    all_input.wait()
    swap_input = copy(land_input.at[1 - core], pair_input, SWAP_INPUT, partner)
    swap_input.start()

    def finish_input(block_of, lanes):
        for half in range(2):
            rows = pl.ds(half * SIDE, SIDE)
            skip = gain[:, pl.ds(lanes, SIDE)] * grad[rows, pl.ds(lanes, SIDE)].astype(F32)
            out_input[rows, pl.ds(lanes, SIDE)] = (block_of(half).T + skip).astype(BF16)

    finish_input(lambda half: land_input[core, pl.ds(half, SIDE, stride=2), :], own)
    swap_input.wait()
    finish_input(lambda half: pair_input[pl.ds(half, SIDE, stride=2), :], other)

    all_filter = copy(land_filter.at[pl.ds(0, 254)], land_filter.at[pl.ds(0, 254)], FILTER, partner)
    all_filter.wait()
    swap_filter = copy(land_filter, pair_filter, SWAP_FILTER, partner)
    swap_filter.start()
    for half in range(2):
        out_filter[pl.ds(half * SIDE, SIDE), pl.ds(own, SIDE)] = land_filter[pl.ds(half, SIDE, stride=2), :].T
    swap_filter.wait()
    for half in range(2):
        out_filter[pl.ds(half * SIDE, SIDE), pl.ds(other, SIDE)] = pair_filter[pl.ds(half, SIDE, stride=2), :].T


def shards(signal, grad_out, filter_taps, skip_gain):
    vmem = pl.BlockSpec(memory_space=pltpu.VMEM)
    held = tables()
    rows = lambda *shape: pltpu.VMEM((*shape, SIDE), F32)
    input_grad, filter_grad = pl.pallas_call(
        body,
        out_shape=(
            pltpu.VMEM((2 * SIDE, 2 * SIDE), BF16),
            pltpu.VMEM((2 * SIDE, 2 * SIDE), F32),
        ),
        in_specs=[pl.BlockSpec(memory_space=pl.ANY)] * 9,
        out_specs=(vmem, vmem),
        scratch_shapes=[
            pltpu.VMEM((2 * SIDE, 2 * SIDE), BF16),
            pltpu.VMEM((2 * SIDE, 2 * SIDE), BF16),
            rows(SIDE),
            pltpu.VMEM((1, 2 * SIDE), F32),
            *(pltpu.VMEM(table.shape, table.dtype) for table in held),
            rows(SIDE), rows(2, 2 * SIDE), rows(2, 2 * SIDE), rows(2 * SIDE), rows(2 * SIDE),
            rows(SIDE), rows(4, SIDE), rows(4, SIDE),
            rows(4, SIDE), rows(SIDE), rows(2, 2 * SIDE), rows(2 * SIDE), rows(2 * SIDE), rows(2 * SIDE),
            pltpu.VMEM((2 * SIDE, 5 * SIDE), F32),
            pltpu.VMEM((5 * SIDE, 2 * SIDE), BF16),
            pltpu.VMEM((5 * SIDE, 2 * SIDE), BF16),
            pltpu.VMEM((5 * SIDE, 2 * SIDE), F32),
            pltpu.VMEM((2 * SIDE, 4 * SIDE), BF16),
            pltpu.VMEM((2 * SIDE, 4 * SIDE), BF16),
            pltpu.SemaphoreType.DMA((9,)),
            pltpu.SemaphoreType.DMA((9,)),
            pltpu.SemaphoreType.DMA((9,)),
        ],
        compiler_params=pltpu.CompilerParams(collective_id=0, has_side_effects=True),
    )(signal[0], grad_out[0], filter_taps, skip_gain[None, :], *held)
    return input_grad[None], filter_grad


def solution(mesh):
    return jax.shard_map(
        shards,
        mesh=mesh,
        in_specs=(P("batch", "seq", None), P("batch", "seq", None), P("seq", None), P()),
        out_specs=(P("batch", "seq", None), P("seq", None)),
        check_vma=False,
    )
```

```python
import ml_dtypes
import numpy as np
import jax
import jax.numpy as jnp
from jax import lax
from jax.experimental import pallas as pl
from jax.experimental.pallas import tpu as pltpu
from jax.sharding import PartitionSpec as P


F32 = jnp.float32
BF16 = jnp.bfloat16
SIDE = 128
LEN = SIDE * SIDE
LOGICAL = pl.DeviceIdType.LOGICAL
TAPS, GRAD, SIGNAL, INPUT, FILTER, SWAP_GRAD, SWAP_SIGNAL, SWAP_INPUT, SWAP_FILTER = range(9)


def split_table(table):
    high = table.astype(np.float32).astype(ml_dtypes.bfloat16)
    low = (table - high.astype(np.float64)).astype(np.float32).astype(ml_dtypes.bfloat16)
    return high, low


def tables():
    index = np.arange(SIDE)
    angle = 2 * np.pi * (np.outer(4 * index + 1, index) % (4 * SIDE)) / (4.0 * SIDE)
    high, low = split_table(np.concatenate([np.cos(angle), -np.sin(angle)], axis=0))
    first = np.concatenate([high, low, high], axis=1)
    fine = 2 * np.pi * (np.outer(index, index) % SIDE) / float(SIDE)
    cos_fine, sin_fine = np.cos(fine), np.sin(fine)
    second = np.stack(split_table(np.block([[cos_fine, -sin_fine], [sin_fine, cos_fine]])))
    third = np.stack(split_table(np.block([[cos_fine, sin_fine], [-sin_fine, cos_fine]])))
    fourth = np.stack(split_table(np.concatenate([np.cos(angle.T), -np.sin(angle.T)], axis=1) / LEN))
    turn = 2 * np.pi * np.outer(4 * index + 1, index) / (4.0 * LEN)
    turns = np.stack([np.cos(turn), np.sin(turn)]).astype(np.float32)
    return tuple(jnp.asarray(table) for table in (first, second, third, fourth, turns))


def split(value):
    high = value.astype(BF16)
    return high, (value - high.astype(F32)).astype(BF16)


def dot(left, right):
    return jnp.dot(left, right, preferred_element_type=F32)


def body(
    signal_far, grad_far, taps_far, gain_far, *rest
):
    (
        tables_far, (out_input, out_filter), (signal, grad, taps, gain), held_tables, rest
    ) = rest[:5], rest[5:7], rest[7:11], rest[11:16], rest[16:]
    run(signal_far, grad_far, taps_far, gain_far, tables_far, out_input, out_filter,
        signal, grad, taps, gain, *held_tables, held_tables, *rest)


def run(
    signal_far, grad_far, taps_far, gain_far, tables_far,
    out_input, out_filter,
    signal, grad, taps, gain, first, second, third, fourth, turns, held_tables,
    send_taps, send_grad, send_signal, stage_grad, stage_signal, land_taps, land_grad, land_signal,
    send_input, send_filter, land_input, land_filter, pair_input, pair_filter,
    coarse, rows_high, rows_low, spectra, columns_high, columns_low,
    sends, recvs, loads,
):
    batch = lax.axis_index("batch")
    seq = lax.axis_index("seq")
    core = batch % 2
    x_low = batch // 2
    x_pos = 2 * ((seq // 8) % 2) + x_low
    y_pos = seq // 16
    z_pos = seq % 8
    me = x_low * 64 + seq
    partner = (batch + 1 - 2 * core) * 64 + seq
    own = pl.multiple_of(core * SIDE, SIDE)
    other = pl.multiple_of((1 - core) * SIDE, SIDE)

    sign = 1 - 2 * core
    bases = []
    for step in range(16):
        x_to = (x_pos + step % 4) % 4
        place = ((y_pos + step // 4) % 4) * 16 + (x_to // 2) * 8
        bases.append((x_to % 2, place, place + (x_to % 2) * 128 + core * 64))

    def each_peer(act):
        def some(near, far, first):
            for dz, start in ((near, 0), (far, first)):
                z_to = (z_pos + sign * dz + 8) % 8
                for x, place, device in bases[start:]:
                    act(x, place + z_to, device + z_to)

        def several(step, carry):
            some(4 - step, 5 + step, 0)
            return carry

        lax.fori_loop(0, 3, several, 0)
        some(1, 0, 1)

    def copy(source, landing, slot, device):
        return pltpu.make_async_remote_copy(
            src_ref=source, dst_ref=landing, send_sem=sends.at[slot], recv_sem=recvs.at[slot],
            device_id=device, device_id_type=LOGICAL,
        )

    def send_all(source_of, landing, slot):
        each_peer(lambda x, s, device: copy(source_of(x, s), landing, slot, device).start())

    x_rows = pl.ds(pl.multiple_of(x_low * SIDE, SIDE), SIDE)
    load_grad, load_signal, load_taps, load_gain, *load_tables = [
        pltpu.make_async_copy(far, near, loads.at[slot])
        for slot, (far, near) in enumerate(
            [
                (grad_far, grad), (signal_far, signal), (taps_far.at[x_rows, pl.ds(own, SIDE)], taps),
                (gain_far, gain), *zip(tables_far, held_tables),
            ]
        )
    ]
    for load in (load_grad, load_signal, load_taps, load_gain, *load_tables):
        load.start()

    barrier = pltpu.get_barrier_semaphore()
    each_peer(
        lambda x, s, device: pl.semaphore_signal(
            barrier, inc=1, device_id=device, device_id_type=LOGICAL
        )
    )
    pl.semaphore_signal(barrier, inc=1, device_id=partner, device_id_type=LOGICAL)

    for load, array, stage, send in (
        (load_grad, grad, stage_grad, send_grad), (load_signal, signal, stage_signal, send_signal)
    ):
        load.wait()
        for half in range(2):
            rows = pl.ds(half * SIDE, SIDE)
            spread = pl.ds(half, SIDE, stride=2)
            stage[spread, :] = array[rows, pl.ds(other, SIDE)].astype(F32).T
            send[core, spread, :] = array[rows, pl.ds(own, SIDE)].astype(F32).T
    load_taps.wait()
    send_taps[...] = taps[...].T
    pl.semaphore_wait(barrier, 128)

    swap_grad = copy(stage_grad, send_grad.at[core], SWAP_GRAD, partner)
    swap_signal = copy(stage_signal, send_signal.at[core], SWAP_SIGNAL, partner)
    swap_grad.start()
    swap_signal.start()

    taps_at = land_taps.at[pl.ds(2 * seq + x_low, 1)]
    send_all(lambda x, s: send_taps.at[pl.ds(64 * x + s, 1)], taps_at, TAPS)
    land_taps[pl.ds(2 * seq + x_low, 1), :] = send_taps[pl.ds(me, 1), :]

    for swap, send, land, slot in (
        (swap_grad, send_grad, land_grad, GRAD),
        (swap_signal, send_signal, land_signal, SIGNAL),
    ):
        swap.wait()
        send_all(
            lambda x, s, send=send: send.at[:, pl.ds(128 * x + 2 * s, 2), :],
            land.at[pl.ds(2 * x_low, 2), pl.ds(2 * seq, 2), :],
            slot,
        )
        for b in range(2):
            land[2 * x_low + b, pl.ds(2 * seq, 2), :] = send[b, pl.ds(2 * me, 2), :]

    all_taps = copy(land_taps.at[pl.ds(0, 127)], land_taps.at[pl.ds(0, 127)], TAPS, partner)
    all_grad, all_signal = (
        copy(land.at[:, pl.ds(0, 127), :], land.at[:, pl.ds(0, 127), :], slot, partner)
        for land, slot in ((land_grad, GRAD), (land_signal, SIGNAL))
    )

    for load in (load_gain, *load_tables):
        load.wait()
    cos_turn, sin_turn = turns[0], turns[1]

    def turn_forward(count):
        for b in range(count):
            real = coarse[:SIDE, b * SIDE : (b + 1) * SIDE]
            imag = coarse[SIDE:, b * SIDE : (b + 1) * SIDE]
            rows = pl.ds(b * SIDE, SIDE)
            rows_high[rows, :SIDE], rows_low[rows, :SIDE] = split(real * cos_turn + imag * sin_turn)
            rows_high[rows, SIDE:], rows_low[rows, SIDE:] = split(imag * cos_turn - real * sin_turn)

    def along_rows(table, count):
        rows = pl.ds(0, count * SIDE)
        return (
            dot(rows_high[rows, :], table[0])
            + dot(rows_low[rows, :], table[0])
            + dot(rows_high[rows, :], table[1])
        )

    def exact_columns(land):
        columns = jnp.concatenate([land[b].astype(BF16) for b in range(4)], axis=1)
        return dot(first[:, : 2 * SIDE], jnp.concatenate([columns, columns], axis=0))

    def inverse(products, count):
        for b in range(count):
            real, imag = products[b]
            rows = pl.ds(b * SIDE, SIDE)
            rows_high[rows, :SIDE], rows_low[rows, :SIDE] = split(real)
            rows_high[rows, SIDE:], rows_low[rows, SIDE:] = split(imag)
        lines = along_rows(third, count)
        for b in range(count):
            real = lines[b * SIDE : (b + 1) * SIDE, :SIDE]
            imag = lines[b * SIDE : (b + 1) * SIDE, SIDE:]
            where = pl.ds(b * SIDE, SIDE)
            columns_high[:SIDE, where], columns_low[:SIDE, where] = split(real * cos_turn - imag * sin_turn)
            columns_high[SIDE:, where], columns_low[SIDE:, where] = split(real * sin_turn + imag * cos_turn)
        where = pl.ds(0, count * SIDE)
        return (
            dot(fourth[0], columns_high[:, where])
            + dot(fourth[0], columns_low[:, where])
            + dot(fourth[1], columns_high[:, where])
        )

    def times_conjugate(left, right):
        return (
            left[0] * right[0] + left[1] * right[1],
            left[1] * right[0] - left[0] * right[1],
        )

    def spectrum(b):
        rows = pl.ds(b * SIDE, SIDE)
        return spectra[rows, :SIDE], spectra[rows, SIDE:]

    all_taps.wait()
    taps_high, taps_low = split(land_taps[...])
    coarse[:, 4 * SIDE :] = dot(first[...], jnp.concatenate([taps_high, taps_high, taps_low], axis=0))
    all_grad.wait()
    coarse[:, : 4 * SIDE] = exact_columns(land_grad)
    turn_forward(5)
    spectra[...] = along_rows(second, 5)
    filter_spectrum = spectrum(4)
    values = inverse([times_conjugate(spectrum(b), filter_spectrum) for b in range(4)], 4)
    for b in range(4):
        send_input[b] = values[:, b * SIDE : (b + 1) * SIDE]
    send_all(
        lambda x, s: send_input.at[pl.ds(2 * x, 2), pl.ds(2 * s, 2), :],
        land_input.at[:, pl.ds(2 * me, 2), :],
        INPUT,
    )
    for b in range(2):
        land_input[b, pl.ds(2 * me, 2), :] = send_input[2 * x_low + b, pl.ds(2 * seq, 2), :]

    all_signal.wait()
    coarse[:, : 4 * SIDE] = exact_columns(land_signal)
    turn_forward(4)
    signal_spectra = along_rows(second, 4)
    total_real, total_imag = 0.0, 0.0
    for b in range(4):
        lines = signal_spectra[b * SIDE : (b + 1) * SIDE]
        real, imag = times_conjugate(spectrum(b), (lines[:, :SIDE], lines[:, SIDE:]))
        total_real, total_imag = total_real + real, total_imag + imag
    send_filter[...] = inverse([(total_real, total_imag)], 1)
    send_all(
        lambda x, s: send_filter.at[pl.ds(2 * s, 2), :], land_filter.at[pl.ds(2 * me, 2), :], FILTER
    )
    land_filter[pl.ds(2 * me, 2), :] = send_filter[pl.ds(2 * seq, 2), :]

    all_input = copy(land_input.at[:, pl.ds(0, 254), :], land_input.at[:, pl.ds(0, 254), :], INPUT, partner)
    all_input.wait()
    swap_input = copy(land_input.at[1 - core], pair_input, SWAP_INPUT, partner)
    swap_input.start()

    def finish_input(block_of, lanes):
        for half in range(2):
            rows = pl.ds(half * SIDE, SIDE)
            skip = gain[:, pl.ds(lanes, SIDE)] * grad[rows, pl.ds(lanes, SIDE)].astype(F32)
            out_input[rows, pl.ds(lanes, SIDE)] = (block_of(half).T + skip).astype(BF16)

    finish_input(lambda half: land_input[core, pl.ds(half, SIDE, stride=2), :], own)
    swap_input.wait()
    finish_input(lambda half: pair_input[pl.ds(half, SIDE, stride=2), :], other)

    all_filter = copy(land_filter.at[pl.ds(0, 254)], land_filter.at[pl.ds(0, 254)], FILTER, partner)
    all_filter.wait()
    swap_filter = copy(land_filter, pair_filter, SWAP_FILTER, partner)
    swap_filter.start()
    for half in range(2):
        out_filter[pl.ds(half * SIDE, SIDE), pl.ds(own, SIDE)] = land_filter[pl.ds(half, SIDE, stride=2), :].T
    swap_filter.wait()
    for half in range(2):
        out_filter[pl.ds(half * SIDE, SIDE), pl.ds(other, SIDE)] = pair_filter[pl.ds(half, SIDE, stride=2), :].T


def shards(signal, grad_out, filter_taps, skip_gain):
    vmem = pl.BlockSpec(memory_space=pltpu.VMEM)
    held = tables()
    rows = lambda *shape: pltpu.VMEM((*shape, SIDE), F32)
    input_grad, filter_grad = pl.pallas_call(
        body,
        out_shape=(
            pltpu.VMEM((2 * SIDE, 2 * SIDE), BF16),
            pltpu.VMEM((2 * SIDE, 2 * SIDE), F32),
        ),
        in_specs=[pl.BlockSpec(memory_space=pl.ANY)] * 9,
        out_specs=(vmem, vmem),
        scratch_shapes=[
            pltpu.VMEM((2 * SIDE, 2 * SIDE), BF16),
            pltpu.VMEM((2 * SIDE, 2 * SIDE), BF16),
            rows(SIDE),
            pltpu.VMEM((1, 2 * SIDE), F32),
            *(pltpu.VMEM(table.shape, table.dtype) for table in held),
            rows(SIDE), rows(2, 2 * SIDE), rows(2, 2 * SIDE), rows(2 * SIDE), rows(2 * SIDE),
            rows(SIDE), rows(4, SIDE), rows(4, SIDE),
            rows(4, SIDE), rows(SIDE), rows(2, 2 * SIDE), rows(2 * SIDE), rows(2 * SIDE), rows(2 * SIDE),
            pltpu.VMEM((2 * SIDE, 5 * SIDE), F32),
            pltpu.VMEM((5 * SIDE, 2 * SIDE), BF16),
            pltpu.VMEM((5 * SIDE, 2 * SIDE), BF16),
            pltpu.VMEM((5 * SIDE, 2 * SIDE), F32),
            pltpu.VMEM((2 * SIDE, 4 * SIDE), BF16),
            pltpu.VMEM((2 * SIDE, 4 * SIDE), BF16),
            pltpu.SemaphoreType.DMA((9,)),
            pltpu.SemaphoreType.DMA((9,)),
            pltpu.SemaphoreType.DMA((9,)),
        ],
        compiler_params=pltpu.CompilerParams(collective_id=0, has_side_effects=True),
    )(signal[0], grad_out[0], filter_taps, skip_gain[None, :], *held)
    return input_grad[None], filter_grad


def solution(mesh):
    return jax.shard_map(
        shards,
        mesh=mesh,
        in_specs=(P("batch", "seq", None), P("batch", "seq", None), P("seq", None), P()),
        out_specs=(P("batch", "seq", None), P("seq", None)),
        check_vma=False,
    )
```

```python
import ml_dtypes
import numpy as np
import jax
import jax.numpy as jnp
from jax import lax
from jax.experimental import pallas as pl
from jax.experimental.pallas import tpu as pltpu
from jax.sharding import PartitionSpec as P


F32 = jnp.float32
BF16 = jnp.bfloat16
SIDE = 128
LEN = SIDE * SIDE
LOGICAL = pl.DeviceIdType.LOGICAL
TAPS, GRAD, SIGNAL, INPUT, FILTER, SWAP_GRAD, SWAP_SIGNAL, SWAP_INPUT, SWAP_FILTER = range(9)


def split_table(table):
    high = table.astype(np.float32).astype(ml_dtypes.bfloat16)
    low = (table - high.astype(np.float64)).astype(np.float32).astype(ml_dtypes.bfloat16)
    return high, low


def tables():
    index = np.arange(SIDE)
    angle = 2 * np.pi * (np.outer(4 * index + 1, index) % (4 * SIDE)) / (4.0 * SIDE)
    high, low = split_table(np.concatenate([np.cos(angle), -np.sin(angle)], axis=0))
    first = np.concatenate([high, low, high], axis=1)
    fine = 2 * np.pi * (np.outer(index, index) % SIDE) / float(SIDE)
    cos_fine, sin_fine = np.cos(fine), np.sin(fine)
    second = np.stack(split_table(np.block([[cos_fine, -sin_fine], [sin_fine, cos_fine]])))
    third = np.stack(split_table(np.block([[cos_fine, sin_fine], [-sin_fine, cos_fine]])))
    fourth = np.stack(split_table(np.concatenate([np.cos(angle.T), -np.sin(angle.T)], axis=1) / LEN))
    turn = 2 * np.pi * np.outer(4 * index + 1, index) / (4.0 * LEN)
    turns = np.stack([np.cos(turn), np.sin(turn)]).astype(np.float32)
    return tuple(jnp.asarray(table) for table in (first, second, third, fourth, turns))


def split(value):
    high = value.astype(BF16)
    return high, (value - high.astype(F32)).astype(BF16)


def dot(left, right):
    return jnp.dot(left, right, preferred_element_type=F32)


def body(
    signal_far, grad_far, taps_far, gain_far, *rest
):
    (
        tables_far, (out_input, out_filter), (signal, grad, taps, gain), held_tables, rest
    ) = rest[:5], rest[5:7], rest[7:11], rest[11:16], rest[16:]
    run(signal_far, grad_far, taps_far, gain_far, tables_far, out_input, out_filter,
        signal, grad, taps, gain, *held_tables, held_tables, *rest)


def run(
    signal_far, grad_far, taps_far, gain_far, tables_far,
    out_input, out_filter,
    signal, grad, taps, gain, first, second, third, fourth, turns, held_tables,
    send_taps, send_grad, send_signal, stage_grad, stage_signal, land_taps, land_grad, land_signal,
    send_input, send_filter, land_input, land_filter, pair_input, pair_filter,
    coarse, rows_high, rows_low, spectra, columns_high, columns_low,
    sends, recvs, loads,
):
    batch = lax.axis_index("batch")
    seq = lax.axis_index("seq")
    core = batch % 2
    x_low = batch // 2
    x_pos = 2 * ((seq // 8) % 2) + x_low
    y_pos = seq // 16
    z_pos = seq % 8
    me = x_low * 64 + seq
    partner = (batch + 1 - 2 * core) * 64 + seq
    own = pl.multiple_of(core * SIDE, SIDE)
    other = pl.multiple_of((1 - core) * SIDE, SIDE)

    sign = 1 - 2 * core
    z_places = [(z_pos + sign * dz + 8) % 8 for dz in (4, 3, 5, 2, 6, 1, 7, 0)]
    x_places = []
    for dx in (2, 3, 1, 0):
        x_to = (x_pos + dx) % 4
        high = (x_to // 2) * 8
        x_places.append((x_to % 2, high, high + (x_to % 2) * 128 + core * 64))

    def each_peer(act):
        def plane(dy, me_too):
            y_place = ((y_pos + dy) % 4) * 16
            places = [y_place + z_to for z_to in z_places]
            for dx in range(4):
                x, high, device = x_places[dx]
                for place in places if dx < 3 or me_too else places[:7]:
                    act(x, place + high, place + device)

        def several(step, carry):
            plane(3 - step, True)
            return carry

        lax.fori_loop(0, 3, several, 0)
        plane(0, False)

    def copy(source, landing, slot, device):
        return pltpu.make_async_remote_copy(
            src_ref=source, dst_ref=landing, send_sem=sends.at[slot], recv_sem=recvs.at[slot],
            device_id=device, device_id_type=LOGICAL,
        )

    def send_all(source_of, landing, slot):
        each_peer(lambda x, s, device: copy(source_of(x, s), landing, slot, device).start())

    x_rows = pl.ds(pl.multiple_of(x_low * SIDE, SIDE), SIDE)
    load_grad, load_signal, load_taps, load_gain, *load_tables = [
        pltpu.make_async_copy(far, near, loads.at[slot])
        for slot, (far, near) in enumerate(
            [
                (grad_far, grad), (signal_far, signal), (taps_far.at[x_rows, pl.ds(own, SIDE)], taps),
                (gain_far, gain), *zip(tables_far, held_tables),
            ]
        )
    ]
    for load in (load_grad, load_signal, load_taps, load_gain, *load_tables):
        load.start()

    barrier = pltpu.get_barrier_semaphore()
    each_peer(
        lambda x, s, device: pl.semaphore_signal(
            barrier, inc=1, device_id=device, device_id_type=LOGICAL
        )
    )
    pl.semaphore_signal(barrier, inc=1, device_id=partner, device_id_type=LOGICAL)

    for load, array, stage, send in (
        (load_grad, grad, stage_grad, send_grad), (load_signal, signal, stage_signal, send_signal)
    ):
        load.wait()
        for half in range(2):
            rows = pl.ds(half * SIDE, SIDE)
            spread = pl.ds(half, SIDE, stride=2)
            stage[spread, :] = array[rows, pl.ds(other, SIDE)].astype(F32).T
            send[core, spread, :] = array[rows, pl.ds(own, SIDE)].astype(F32).T
    load_taps.wait()
    send_taps[...] = taps[...].T
    pl.semaphore_wait(barrier, 128)

    swap_grad = copy(stage_grad, send_grad.at[core], SWAP_GRAD, partner)
    swap_signal = copy(stage_signal, send_signal.at[core], SWAP_SIGNAL, partner)
    swap_grad.start()
    swap_signal.start()

    taps_at = land_taps.at[pl.ds(2 * seq + x_low, 1)]
    send_all(lambda x, s: send_taps.at[pl.ds(64 * x + s, 1)], taps_at, TAPS)
    land_taps[pl.ds(2 * seq + x_low, 1), :] = send_taps[pl.ds(me, 1), :]

    for swap, send, land, slot in (
        (swap_grad, send_grad, land_grad, GRAD),
        (swap_signal, send_signal, land_signal, SIGNAL),
    ):
        swap.wait()
        send_all(
            lambda x, s, send=send: send.at[:, pl.ds(128 * x + 2 * s, 2), :],
            land.at[pl.ds(2 * x_low, 2), pl.ds(2 * seq, 2), :],
            slot,
        )
        for b in range(2):
            land[2 * x_low + b, pl.ds(2 * seq, 2), :] = send[b, pl.ds(2 * me, 2), :]

    all_taps = copy(land_taps.at[pl.ds(0, 127)], land_taps.at[pl.ds(0, 127)], TAPS, partner)
    all_grad, all_signal = (
        copy(land.at[:, pl.ds(0, 127), :], land.at[:, pl.ds(0, 127), :], slot, partner)
        for land, slot in ((land_grad, GRAD), (land_signal, SIGNAL))
    )

    for load in (load_gain, *load_tables):
        load.wait()
    cos_turn, sin_turn = turns[0], turns[1]

    def turn_forward(count):
        for b in range(count):
            real = coarse[:SIDE, b * SIDE : (b + 1) * SIDE]
            imag = coarse[SIDE:, b * SIDE : (b + 1) * SIDE]
            rows = pl.ds(b * SIDE, SIDE)
            rows_high[rows, :SIDE], rows_low[rows, :SIDE] = split(real * cos_turn + imag * sin_turn)
            rows_high[rows, SIDE:], rows_low[rows, SIDE:] = split(imag * cos_turn - real * sin_turn)

    def along_rows(table, count):
        rows = pl.ds(0, count * SIDE)
        return (
            dot(rows_high[rows, :], table[0])
            + dot(rows_low[rows, :], table[0])
            + dot(rows_high[rows, :], table[1])
        )

    def exact_columns(land):
        columns = jnp.concatenate([land[b].astype(BF16) for b in range(4)], axis=1)
        return dot(first[:, : 2 * SIDE], jnp.concatenate([columns, columns], axis=0))

    def inverse(products, count):
        for b in range(count):
            real, imag = products[b]
            rows = pl.ds(b * SIDE, SIDE)
            rows_high[rows, :SIDE], rows_low[rows, :SIDE] = split(real)
            rows_high[rows, SIDE:], rows_low[rows, SIDE:] = split(imag)
        lines = along_rows(third, count)
        for b in range(count):
            real = lines[b * SIDE : (b + 1) * SIDE, :SIDE]
            imag = lines[b * SIDE : (b + 1) * SIDE, SIDE:]
            where = pl.ds(b * SIDE, SIDE)
            columns_high[:SIDE, where], columns_low[:SIDE, where] = split(real * cos_turn - imag * sin_turn)
            columns_high[SIDE:, where], columns_low[SIDE:, where] = split(real * sin_turn + imag * cos_turn)
        where = pl.ds(0, count * SIDE)
        return (
            dot(fourth[0], columns_high[:, where])
            + dot(fourth[0], columns_low[:, where])
            + dot(fourth[1], columns_high[:, where])
        )

    def times_conjugate(left, right):
        return (
            left[0] * right[0] + left[1] * right[1],
            left[1] * right[0] - left[0] * right[1],
        )

    def spectrum(b):
        rows = pl.ds(b * SIDE, SIDE)
        return spectra[rows, :SIDE], spectra[rows, SIDE:]

    all_taps.wait()
    taps_high, taps_low = split(land_taps[...])
    coarse[:, 4 * SIDE :] = dot(first[...], jnp.concatenate([taps_high, taps_high, taps_low], axis=0))
    all_grad.wait()
    coarse[:, : 4 * SIDE] = exact_columns(land_grad)
    turn_forward(5)
    spectra[...] = along_rows(second, 5)
    filter_spectrum = spectrum(4)
    values = inverse([times_conjugate(spectrum(b), filter_spectrum) for b in range(4)], 4)
    for b in range(4):
        send_input[b] = values[:, b * SIDE : (b + 1) * SIDE]
    send_all(
        lambda x, s: send_input.at[pl.ds(2 * x, 2), pl.ds(2 * s, 2), :],
        land_input.at[:, pl.ds(2 * me, 2), :],
        INPUT,
    )
    for b in range(2):
        land_input[b, pl.ds(2 * me, 2), :] = send_input[2 * x_low + b, pl.ds(2 * seq, 2), :]

    all_signal.wait()
    coarse[:, : 4 * SIDE] = exact_columns(land_signal)
    turn_forward(4)
    signal_spectra = along_rows(second, 4)
    total_real, total_imag = 0.0, 0.0
    for b in range(4):
        lines = signal_spectra[b * SIDE : (b + 1) * SIDE]
        real, imag = times_conjugate(spectrum(b), (lines[:, :SIDE], lines[:, SIDE:]))
        total_real, total_imag = total_real + real, total_imag + imag
    send_filter[...] = inverse([(total_real, total_imag)], 1)
    send_all(
        lambda x, s: send_filter.at[pl.ds(2 * s, 2), :], land_filter.at[pl.ds(2 * me, 2), :], FILTER
    )
    land_filter[pl.ds(2 * me, 2), :] = send_filter[pl.ds(2 * seq, 2), :]

    all_input = copy(land_input.at[:, pl.ds(0, 254), :], land_input.at[:, pl.ds(0, 254), :], INPUT, partner)
    all_input.wait()
    swap_input = copy(land_input.at[1 - core], pair_input, SWAP_INPUT, partner)
    swap_input.start()

    def finish_input(block_of, lanes):
        for half in range(2):
            rows = pl.ds(half * SIDE, SIDE)
            skip = gain[:, pl.ds(lanes, SIDE)] * grad[rows, pl.ds(lanes, SIDE)].astype(F32)
            out_input[rows, pl.ds(lanes, SIDE)] = (block_of(half).T + skip).astype(BF16)

    finish_input(lambda half: land_input[core, pl.ds(half, SIDE, stride=2), :], own)
    swap_input.wait()
    finish_input(lambda half: pair_input[pl.ds(half, SIDE, stride=2), :], other)

    all_filter = copy(land_filter.at[pl.ds(0, 254)], land_filter.at[pl.ds(0, 254)], FILTER, partner)
    all_filter.wait()
    swap_filter = copy(land_filter, pair_filter, SWAP_FILTER, partner)
    swap_filter.start()
    for half in range(2):
        out_filter[pl.ds(half * SIDE, SIDE), pl.ds(own, SIDE)] = land_filter[pl.ds(half, SIDE, stride=2), :].T
    swap_filter.wait()
    for half in range(2):
        out_filter[pl.ds(half * SIDE, SIDE), pl.ds(other, SIDE)] = pair_filter[pl.ds(half, SIDE, stride=2), :].T


def put_out(input_near, filter_near, input_far, filter_far, sems):
    copies = [
        pltpu.make_async_copy(filter_near, filter_far, sems.at[0]),
        pltpu.make_async_copy(input_near, input_far, sems.at[1]),
    ]
    for copy in copies:
        copy.start()
    for copy in copies:
        copy.wait()


def shards(signal, grad_out, filter_taps, skip_gain):
    vmem = pl.BlockSpec(memory_space=pltpu.VMEM)
    held = tables()
    rows = lambda *shape: pltpu.VMEM((*shape, SIDE), F32)
    input_grad, filter_grad = pl.pallas_call(
        body,
        out_shape=(
            pltpu.VMEM((2 * SIDE, 2 * SIDE), BF16),
            pltpu.VMEM((2 * SIDE, 2 * SIDE), F32),
        ),
        in_specs=[pl.BlockSpec(memory_space=pl.ANY)] * 9,
        out_specs=(vmem, vmem),
        scratch_shapes=[
            pltpu.VMEM((2 * SIDE, 2 * SIDE), BF16),
            pltpu.VMEM((2 * SIDE, 2 * SIDE), BF16),
            rows(SIDE),
            pltpu.VMEM((1, 2 * SIDE), F32),
            *(pltpu.VMEM(table.shape, table.dtype) for table in held),
            rows(SIDE), rows(2, 2 * SIDE), rows(2, 2 * SIDE), rows(2 * SIDE), rows(2 * SIDE),
            rows(SIDE), rows(4, SIDE), rows(4, SIDE),
            rows(4, SIDE), rows(SIDE), rows(2, 2 * SIDE), rows(2 * SIDE), rows(2 * SIDE), rows(2 * SIDE),
            pltpu.VMEM((2 * SIDE, 5 * SIDE), F32),
            pltpu.VMEM((5 * SIDE, 2 * SIDE), BF16),
            pltpu.VMEM((5 * SIDE, 2 * SIDE), BF16),
            pltpu.VMEM((5 * SIDE, 2 * SIDE), F32),
            pltpu.VMEM((2 * SIDE, 4 * SIDE), BF16),
            pltpu.VMEM((2 * SIDE, 4 * SIDE), BF16),
            pltpu.SemaphoreType.DMA((9,)),
            pltpu.SemaphoreType.DMA((9,)),
            pltpu.SemaphoreType.DMA((9,)),
        ],
        compiler_params=pltpu.CompilerParams(collective_id=0, has_side_effects=True),
    )(signal[0], grad_out[0], filter_taps, skip_gain[None, :], *held)
    place = pl.BlockSpec(memory_space=pl.ANY)
    input_grad, filter_grad = pl.pallas_call(
        put_out,
        out_shape=(
            jax.ShapeDtypeStruct((2 * SIDE, 2 * SIDE), BF16),
            jax.ShapeDtypeStruct((2 * SIDE, 2 * SIDE), F32),
        ),
        in_specs=[vmem] * 2,
        out_specs=(place, place),
        scratch_shapes=[pltpu.SemaphoreType.DMA((2,))],
    )(*(pltpu.with_memory_space_constraint(x, pltpu.VMEM) for x in (input_grad, filter_grad)))
    return input_grad[None], filter_grad


def solution(mesh):
    return jax.shard_map(
        shards,
        mesh=mesh,
        in_specs=(P("batch", "seq", None), P("batch", "seq", None), P("seq", None), P()),
        out_specs=(P("batch", "seq", None), P("seq", None)),
        check_vma=False,
    )
```

```python
import ml_dtypes
import numpy as np
import jax
import jax.numpy as jnp
from jax import lax
from jax.experimental import pallas as pl
from jax.experimental.pallas import tpu as pltpu
from jax.sharding import PartitionSpec as P


F32 = jnp.float32
BF16 = jnp.bfloat16
SIDE = 128
LEN = SIDE * SIDE
LOGICAL = pl.DeviceIdType.LOGICAL
TAPS, GRAD, SIGNAL, INPUT, FILTER, SWAP_GRAD, SWAP_SIGNAL, SWAP_INPUT, SWAP_FILTER = range(9)


ORDER = sorted(
    [(dx, dy, dz) for dz in range(8) for dy in range(4) for dx in range(4) if dx + dy + dz],
    key=lambda d: (-sum(min(step, size - step) for step, size in zip(d, (4, 4, 8))), min(d[2], 8 - d[2])),
)


def split_table(table):
    high = table.astype(np.float32).astype(ml_dtypes.bfloat16)
    low = (table - high.astype(np.float64)).astype(np.float32).astype(ml_dtypes.bfloat16)
    return high, low


def tables():
    index = np.arange(SIDE)
    angle = 2 * np.pi * (np.outer(4 * index + 1, index) % (4 * SIDE)) / (4.0 * SIDE)
    high, low = split_table(np.concatenate([np.cos(angle), -np.sin(angle)], axis=0))
    first = np.concatenate([high, low, high], axis=1)
    fine = 2 * np.pi * (np.outer(index, index) % SIDE) / float(SIDE)
    cos_fine, sin_fine = np.cos(fine), np.sin(fine)
    second = np.stack(split_table(np.block([[cos_fine, -sin_fine], [sin_fine, cos_fine]])))
    third = np.stack(split_table(np.block([[cos_fine, sin_fine], [-sin_fine, cos_fine]])))
    fourth = np.stack(split_table(np.concatenate([np.cos(angle.T), -np.sin(angle.T)], axis=1) / LEN))
    turn = 2 * np.pi * np.outer(4 * index + 1, index) / (4.0 * LEN)
    turns = np.stack([np.cos(turn), np.sin(turn)]).astype(np.float32)
    return tuple(jnp.asarray(table) for table in (first, second, third, fourth, turns))


def split(value):
    high = value.astype(BF16)
    return high, (value - high.astype(F32)).astype(BF16)


def dot(left, right):
    return jnp.dot(left, right, preferred_element_type=F32)


def body(
    signal_far, grad_far, taps_far, gain_far, *rest
):
    (
        tables_far, (out_input, out_filter), (signal, grad, taps, gain), held_tables, rest
    ) = rest[:5], rest[5:7], rest[7:11], rest[11:16], rest[16:]
    run(signal_far, grad_far, taps_far, gain_far, tables_far, out_input, out_filter,
        signal, grad, taps, gain, *held_tables, held_tables, *rest)


def run(
    signal_far, grad_far, taps_far, gain_far, tables_far,
    out_input, out_filter,
    signal, grad, taps, gain, first, second, third, fourth, turns, held_tables,
    send_taps, send_grad, send_signal, stage_grad, stage_signal, land_taps, land_grad, land_signal,
    send_input, send_filter, land_input, land_filter, pair_input, pair_filter,
    coarse, rows_high, rows_low, spectra, columns_high, columns_low,
    sends, recvs, loads,
):
    batch = lax.axis_index("batch")
    seq = lax.axis_index("seq")
    core = batch % 2
    x_low = batch // 2
    x_pos = 2 * ((seq // 8) % 2) + x_low
    y_pos = seq // 16
    z_pos = seq % 8
    me = x_low * 64 + seq
    partner = (batch + 1 - 2 * core) * 64 + seq
    own = pl.multiple_of(core * SIDE, SIDE)
    other = pl.multiple_of((1 - core) * SIDE, SIDE)

    sign = 1 - 2 * core
    z_places = [(z_pos + sign * dz + 8) % 8 for dz in range(8)]
    y_places = [((y_pos + dy) % 4) * 16 for dy in range(4)]
    x_places = []
    for dx in range(4):
        x_to = (x_pos + dx) % 4
        high = (x_to // 2) * 8
        x_places.append((x_to % 2, high, high + (x_to % 2) * 128 + core * 64))

    def each_peer(act):
        for dx, dy, dz in ORDER:
            place = y_places[dy] + z_places[dz]
            x, high, device = x_places[dx]
            act(x, place + high, place + device)

    def copy(source, landing, slot, device):
        return pltpu.make_async_remote_copy(
            src_ref=source, dst_ref=landing, send_sem=sends.at[slot], recv_sem=recvs.at[slot],
            device_id=device, device_id_type=LOGICAL,
        )

    def send_all(source_of, landing, slot):
        each_peer(lambda x, s, device: copy(source_of(x, s), landing, slot, device).start())

    x_rows = pl.ds(pl.multiple_of(x_low * SIDE, SIDE), SIDE)
    load_grad, load_signal, load_taps, load_gain, *load_tables = [
        pltpu.make_async_copy(far, near, loads.at[slot])
        for slot, (far, near) in enumerate(
            [
                (grad_far, grad), (signal_far, signal), (taps_far.at[x_rows, pl.ds(own, SIDE)], taps),
                (gain_far, gain), *zip(tables_far, held_tables),
            ]
        )
    ]
    for load in (load_grad, load_signal, load_taps, load_gain, *load_tables):
        load.start()

    barrier = pltpu.get_barrier_semaphore()
    each_peer(
        lambda x, s, device: pl.semaphore_signal(
            barrier, inc=1, device_id=device, device_id_type=LOGICAL
        )
    )
    pl.semaphore_signal(barrier, inc=1, device_id=partner, device_id_type=LOGICAL)

    for load, array, stage, send in (
        (load_grad, grad, stage_grad, send_grad), (load_signal, signal, stage_signal, send_signal)
    ):
        load.wait()
        for half in range(2):
            rows = pl.ds(half * SIDE, SIDE)
            spread = pl.ds(half, SIDE, stride=2)
            stage[spread, :] = array[rows, pl.ds(other, SIDE)].astype(F32).T
            send[core, spread, :] = array[rows, pl.ds(own, SIDE)].astype(F32).T
    load_taps.wait()
    send_taps[...] = taps[...].T
    pl.semaphore_wait(barrier, 128)

    swap_grad = copy(stage_grad, send_grad.at[core], SWAP_GRAD, partner)
    swap_signal = copy(stage_signal, send_signal.at[core], SWAP_SIGNAL, partner)
    swap_grad.start()
    swap_signal.start()

    taps_at = land_taps.at[pl.ds(2 * seq + x_low, 1)]
    send_all(lambda x, s: send_taps.at[pl.ds(64 * x + s, 1)], taps_at, TAPS)
    land_taps[pl.ds(2 * seq + x_low, 1), :] = send_taps[pl.ds(me, 1), :]

    for swap, send, land, slot in (
        (swap_grad, send_grad, land_grad, GRAD),
        (swap_signal, send_signal, land_signal, SIGNAL),
    ):
        swap.wait()
        send_all(
            lambda x, s, send=send: send.at[:, pl.ds(128 * x + 2 * s, 2), :],
            land.at[pl.ds(2 * x_low, 2), pl.ds(2 * seq, 2), :],
            slot,
        )
        for b in range(2):
            land[2 * x_low + b, pl.ds(2 * seq, 2), :] = send[b, pl.ds(2 * me, 2), :]

    all_taps = copy(land_taps.at[pl.ds(0, 127)], land_taps.at[pl.ds(0, 127)], TAPS, partner)
    all_grad, all_signal = (
        copy(land.at[:, pl.ds(0, 127), :], land.at[:, pl.ds(0, 127), :], slot, partner)
        for land, slot in ((land_grad, GRAD), (land_signal, SIGNAL))
    )

    for load in (load_gain, *load_tables):
        load.wait()
    cos_turn, sin_turn = turns[0], turns[1]

    def turn_forward(count):
        for b in range(count):
            real = coarse[:SIDE, b * SIDE : (b + 1) * SIDE]
            imag = coarse[SIDE:, b * SIDE : (b + 1) * SIDE]
            rows = pl.ds(b * SIDE, SIDE)
            rows_high[rows, :SIDE], rows_low[rows, :SIDE] = split(real * cos_turn + imag * sin_turn)
            rows_high[rows, SIDE:], rows_low[rows, SIDE:] = split(imag * cos_turn - real * sin_turn)

    def along_rows(table, count):
        rows = pl.ds(0, count * SIDE)
        return (
            dot(rows_high[rows, :], table[0])
            + dot(rows_low[rows, :], table[0])
            + dot(rows_high[rows, :], table[1])
        )

    def exact_columns(land):
        columns = jnp.concatenate([land[b].astype(BF16) for b in range(4)], axis=1)
        return dot(first[:, : 2 * SIDE], jnp.concatenate([columns, columns], axis=0))

    def inverse(products, count):
        for b in range(count):
            real, imag = products[b]
            rows = pl.ds(b * SIDE, SIDE)
            rows_high[rows, :SIDE], rows_low[rows, :SIDE] = split(real)
            rows_high[rows, SIDE:], rows_low[rows, SIDE:] = split(imag)
        lines = along_rows(third, count)
        for b in range(count):
            real = lines[b * SIDE : (b + 1) * SIDE, :SIDE]
            imag = lines[b * SIDE : (b + 1) * SIDE, SIDE:]
            where = pl.ds(b * SIDE, SIDE)
            columns_high[:SIDE, where], columns_low[:SIDE, where] = split(real * cos_turn - imag * sin_turn)
            columns_high[SIDE:, where], columns_low[SIDE:, where] = split(real * sin_turn + imag * cos_turn)
        where = pl.ds(0, count * SIDE)
        return (
            dot(fourth[0], columns_high[:, where])
            + dot(fourth[0], columns_low[:, where])
            + dot(fourth[1], columns_high[:, where])
        )

    def times_conjugate(left, right):
        return (
            left[0] * right[0] + left[1] * right[1],
            left[1] * right[0] - left[0] * right[1],
        )

    def spectrum(b):
        rows = pl.ds(b * SIDE, SIDE)
        return spectra[rows, :SIDE], spectra[rows, SIDE:]

    all_taps.wait()
    taps_high, taps_low = split(land_taps[...])
    coarse[:, 4 * SIDE :] = dot(first[...], jnp.concatenate([taps_high, taps_high, taps_low], axis=0))
    all_grad.wait()
    coarse[:, : 4 * SIDE] = exact_columns(land_grad)
    turn_forward(5)
    spectra[...] = along_rows(second, 5)
    filter_spectrum = spectrum(4)
    values = inverse([times_conjugate(spectrum(b), filter_spectrum) for b in range(4)], 4)
    for b in range(4):
        send_input[b] = values[:, b * SIDE : (b + 1) * SIDE]
    send_all(
        lambda x, s: send_input.at[pl.ds(2 * x, 2), pl.ds(2 * s, 2), :],
        land_input.at[:, pl.ds(2 * me, 2), :],
        INPUT,
    )
    for b in range(2):
        land_input[b, pl.ds(2 * me, 2), :] = send_input[2 * x_low + b, pl.ds(2 * seq, 2), :]

    all_signal.wait()
    coarse[:, : 4 * SIDE] = exact_columns(land_signal)
    turn_forward(4)
    signal_spectra = along_rows(second, 4)
    total_real, total_imag = 0.0, 0.0
    for b in range(4):
        lines = signal_spectra[b * SIDE : (b + 1) * SIDE]
        real, imag = times_conjugate(spectrum(b), (lines[:, :SIDE], lines[:, SIDE:]))
        total_real, total_imag = total_real + real, total_imag + imag
    send_filter[...] = inverse([(total_real, total_imag)], 1)
    send_all(
        lambda x, s: send_filter.at[pl.ds(2 * s, 2), :], land_filter.at[pl.ds(2 * me, 2), :], FILTER
    )
    land_filter[pl.ds(2 * me, 2), :] = send_filter[pl.ds(2 * seq, 2), :]

    all_input = copy(land_input.at[:, pl.ds(0, 254), :], land_input.at[:, pl.ds(0, 254), :], INPUT, partner)
    all_input.wait()
    swap_input = copy(land_input.at[1 - core], pair_input, SWAP_INPUT, partner)
    swap_input.start()

    def finish_input(block_of, lanes):
        for half in range(2):
            rows = pl.ds(half * SIDE, SIDE)
            skip = gain[:, pl.ds(lanes, SIDE)] * grad[rows, pl.ds(lanes, SIDE)].astype(F32)
            out_input[rows, pl.ds(lanes, SIDE)] = (block_of(half).T + skip).astype(BF16)

    finish_input(lambda half: land_input[core, pl.ds(half, SIDE, stride=2), :], own)
    swap_input.wait()
    finish_input(lambda half: pair_input[pl.ds(half, SIDE, stride=2), :], other)

    all_filter = copy(land_filter.at[pl.ds(0, 254)], land_filter.at[pl.ds(0, 254)], FILTER, partner)
    all_filter.wait()
    swap_filter = copy(land_filter, pair_filter, SWAP_FILTER, partner)
    swap_filter.start()
    for half in range(2):
        out_filter[pl.ds(half * SIDE, SIDE), pl.ds(own, SIDE)] = land_filter[pl.ds(half, SIDE, stride=2), :].T
    swap_filter.wait()
    for half in range(2):
        out_filter[pl.ds(half * SIDE, SIDE), pl.ds(other, SIDE)] = pair_filter[pl.ds(half, SIDE, stride=2), :].T


def put_out(input_near, filter_near, input_far, filter_far, sems):
    copies = [
        pltpu.make_async_copy(filter_near, filter_far, sems.at[0]),
        pltpu.make_async_copy(input_near, input_far, sems.at[1]),
    ]
    for copy in copies:
        copy.start()
    for copy in copies:
        copy.wait()


def shards(signal, grad_out, filter_taps, skip_gain):
    vmem = pl.BlockSpec(memory_space=pltpu.VMEM)
    held = tables()
    rows = lambda *shape: pltpu.VMEM((*shape, SIDE), F32)
    input_grad, filter_grad = pl.pallas_call(
        body,
        out_shape=(
            pltpu.VMEM((2 * SIDE, 2 * SIDE), BF16),
            pltpu.VMEM((2 * SIDE, 2 * SIDE), F32),
        ),
        in_specs=[pl.BlockSpec(memory_space=pl.ANY)] * 9,
        out_specs=(vmem, vmem),
        scratch_shapes=[
            pltpu.VMEM((2 * SIDE, 2 * SIDE), BF16),
            pltpu.VMEM((2 * SIDE, 2 * SIDE), BF16),
            rows(SIDE),
            pltpu.VMEM((1, 2 * SIDE), F32),
            *(pltpu.VMEM(table.shape, table.dtype) for table in held),
            rows(SIDE), rows(2, 2 * SIDE), rows(2, 2 * SIDE), rows(2 * SIDE), rows(2 * SIDE),
            rows(SIDE), rows(4, SIDE), rows(4, SIDE),
            rows(4, SIDE), rows(SIDE), rows(2, 2 * SIDE), rows(2 * SIDE), rows(2 * SIDE), rows(2 * SIDE),
            pltpu.VMEM((2 * SIDE, 5 * SIDE), F32),
            pltpu.VMEM((5 * SIDE, 2 * SIDE), BF16),
            pltpu.VMEM((5 * SIDE, 2 * SIDE), BF16),
            pltpu.VMEM((5 * SIDE, 2 * SIDE), F32),
            pltpu.VMEM((2 * SIDE, 4 * SIDE), BF16),
            pltpu.VMEM((2 * SIDE, 4 * SIDE), BF16),
            pltpu.SemaphoreType.DMA((9,)),
            pltpu.SemaphoreType.DMA((9,)),
            pltpu.SemaphoreType.DMA((9,)),
        ],
        compiler_params=pltpu.CompilerParams(collective_id=0, has_side_effects=True),
    )(signal[0], grad_out[0], filter_taps, skip_gain[None, :], *held)
    place = pl.BlockSpec(memory_space=pl.ANY)
    input_grad, filter_grad = pl.pallas_call(
        put_out,
        out_shape=(
            jax.ShapeDtypeStruct((2 * SIDE, 2 * SIDE), BF16),
            jax.ShapeDtypeStruct((2 * SIDE, 2 * SIDE), F32),
        ),
        in_specs=[vmem] * 2,
        out_specs=(place, place),
        scratch_shapes=[pltpu.SemaphoreType.DMA((2,))],
    )(*(pltpu.with_memory_space_constraint(x, pltpu.VMEM) for x in (input_grad, filter_grad)))
    return input_grad[None], filter_grad


def solution(mesh):
    return jax.shard_map(
        shards,
        mesh=mesh,
        in_specs=(P("batch", "seq", None), P("batch", "seq", None), P("seq", None), P()),
        out_specs=(P("batch", "seq", None), P("seq", None)),
        check_vma=False,
    )
```

```python
import ml_dtypes
import numpy as np
import jax
import jax.numpy as jnp
from jax import lax
from jax.experimental import pallas as pl
from jax.experimental.pallas import tpu as pltpu
from jax.sharding import PartitionSpec as P


F32 = jnp.float32
BF16 = jnp.bfloat16
SIDE = 128
LEN = SIDE * SIDE
LOGICAL = pl.DeviceIdType.LOGICAL
TAPS, GRAD, SIGNAL, INPUT, FILTER, SWAP_GRAD, SWAP_SIGNAL, SWAP_INPUT, SWAP_FILTER = range(9)


ORDER = sorted(
    [(dx, dy, dz) for dz in range(8) for dy in range(4) for dx in range(4) if dx + dy + dz],
    key=lambda d: (-sum(min(step, size - step) for step, size in zip(d, (4, 4, 8))), min(d[2], 8 - d[2])),
)


def split_table(table):
    high = table.astype(np.float32).astype(ml_dtypes.bfloat16)
    low = (table - high.astype(np.float64)).astype(np.float32).astype(ml_dtypes.bfloat16)
    return high, low


def tables():
    index = np.arange(SIDE)
    angle = 2 * np.pi * (np.outer(4 * index + 1, index) % (4 * SIDE)) / (4.0 * SIDE)
    high, low = split_table(np.concatenate([np.cos(angle), -np.sin(angle)], axis=0))
    first = np.concatenate([high, low, high], axis=1)
    fine = 2 * np.pi * (np.outer(index, index) % SIDE) / float(SIDE)
    cos_fine, sin_fine = np.cos(fine), np.sin(fine)
    second = np.stack(split_table(np.block([[cos_fine, -sin_fine], [sin_fine, cos_fine]])))
    third = np.stack(split_table(np.block([[cos_fine, sin_fine], [-sin_fine, cos_fine]])))
    fourth = np.stack(split_table(np.concatenate([np.cos(angle.T), -np.sin(angle.T)], axis=1) / LEN))
    turn = 2 * np.pi * np.outer(4 * index + 1, index) / (4.0 * LEN)
    turns = np.stack([np.cos(turn), np.sin(turn)]).astype(np.float32)
    return tuple(jnp.asarray(table) for table in (first, second, third, fourth, turns))


def split(value):
    high = value.astype(BF16)
    return high, (value - high.astype(F32)).astype(BF16)


def dot(left, right):
    return jnp.dot(left, right, preferred_element_type=F32)


def body(
    signal_far, grad_far, taps_far, gain_far, *rest
):
    (
        tables_far, (out_input, out_filter), (signal, grad, taps, gain), held_tables, rest
    ) = rest[:5], rest[5:7], rest[7:11], rest[11:16], rest[16:]
    run(signal_far, grad_far, taps_far, gain_far, tables_far, out_input, out_filter,
        signal, grad, taps, gain, *held_tables, held_tables, *rest)


def run(
    signal_far, grad_far, taps_far, gain_far, tables_far,
    out_input, out_filter,
    signal, grad, taps, gain, first, second, third, fourth, turns, held_tables,
    send_taps, send_grad, send_signal, stage_grad, stage_signal, land_taps, land_grad, land_signal,
    send_input, send_filter, land_input, land_filter, pair_input, pair_filter,
    coarse, rows_high, rows_low, spectra, columns_high, columns_low,
    sends, recvs, loads,
):
    batch = lax.axis_index("batch")
    seq = lax.axis_index("seq")
    core = batch % 2
    x_low = batch // 2
    x_pos = 2 * ((seq // 8) % 2) + x_low
    y_pos = seq // 16
    z_pos = seq % 8
    me = x_low * 64 + seq
    partner = (batch + 1 - 2 * core) * 64 + seq
    own = pl.multiple_of(core * SIDE, SIDE)
    other = pl.multiple_of((1 - core) * SIDE, SIDE)

    sign = 1 - 2 * core
    z_places = [(z_pos + sign * dz + 8) % 8 for dz in range(8)]
    y_places = [((y_pos + dy) % 4) * 16 for dy in range(4)]
    x_places = []
    for dx in range(4):
        x_to = (x_pos + dx) % 4
        high = (x_to // 2) * 8
        x_places.append((x_to % 2, high, high + (x_to % 2) * 128 + core * 64))

    def each_peer(act):
        for dx, dy, dz in ORDER:
            place = y_places[dy] + z_places[dz]
            x, high, device = x_places[dx]
            act(x, place + high, place + device)

    def copy(source, landing, slot, device):
        return pltpu.make_async_remote_copy(
            src_ref=source, dst_ref=landing, send_sem=sends.at[slot], recv_sem=recvs.at[slot],
            device_id=device, device_id_type=LOGICAL,
        )

    def send_all(source_of, landing, slot):
        each_peer(lambda x, s, device: copy(source_of(x, s), landing, slot, device).start())

    x_rows = pl.ds(pl.multiple_of(x_low * SIDE, SIDE), SIDE)
    load_grad, load_signal, load_taps, load_gain, *load_tables = [
        pltpu.make_async_copy(far, near, loads.at[slot])
        for slot, (far, near) in enumerate(
            [
                (grad_far, grad), (signal_far, signal), (taps_far.at[x_rows, pl.ds(own, SIDE)], taps),
                (gain_far, gain), *zip(tables_far, held_tables),
            ]
        )
    ]
    for load in (load_grad, load_signal, load_taps, load_gain, *load_tables):
        load.start()

    barrier = pltpu.get_barrier_semaphore()
    each_peer(
        lambda x, s, device: pl.semaphore_signal(
            barrier, inc=1, device_id=device, device_id_type=LOGICAL
        )
    )
    pl.semaphore_signal(barrier, inc=1, device_id=partner, device_id_type=LOGICAL)

    for load, array, stage, send in (
        (load_grad, grad, stage_grad, send_grad), (load_signal, signal, stage_signal, send_signal)
    ):
        load.wait()
        for half in range(2):
            rows = pl.ds(half * SIDE, SIDE)
            spread = pl.ds(half, SIDE, stride=2)
            stage[spread, :] = array[rows, pl.ds(other, SIDE)].astype(F32).T
            send[core, spread, :] = array[rows, pl.ds(own, SIDE)].astype(F32).T
    load_taps.wait()
    send_taps[...] = taps[...].T
    pl.semaphore_wait(barrier, 128)

    swap_grad = copy(stage_grad, send_grad.at[core], SWAP_GRAD, partner)
    swap_signal = copy(stage_signal, send_signal.at[core], SWAP_SIGNAL, partner)
    swap_grad.start()

    taps_at = land_taps.at[pl.ds(2 * seq + x_low, 1)]
    send_all(lambda x, s: send_taps.at[pl.ds(64 * x + s, 1)], taps_at, TAPS)
    land_taps[pl.ds(2 * seq + x_low, 1), :] = send_taps[pl.ds(me, 1), :]

    for swap, send, land, slot in (
        (swap_grad, send_grad, land_grad, GRAD),
        (swap_signal, send_signal, land_signal, SIGNAL),
    ):
        swap.wait()
        if slot == GRAD:
            swap_signal.start()
        send_all(
            lambda x, s, send=send: send.at[:, pl.ds(128 * x + 2 * s, 2), :],
            land.at[pl.ds(2 * x_low, 2), pl.ds(2 * seq, 2), :],
            slot,
        )
        for b in range(2):
            land[2 * x_low + b, pl.ds(2 * seq, 2), :] = send[b, pl.ds(2 * me, 2), :]

    all_taps = copy(land_taps.at[pl.ds(0, 127)], land_taps.at[pl.ds(0, 127)], TAPS, partner)
    all_grad, all_signal = (
        copy(land.at[:, pl.ds(0, 127), :], land.at[:, pl.ds(0, 127), :], slot, partner)
        for land, slot in ((land_grad, GRAD), (land_signal, SIGNAL))
    )

    for load in (load_gain, *load_tables):
        load.wait()
    cos_turn, sin_turn = turns[0], turns[1]

    def turn_forward(count):
        for b in range(count):
            real = coarse[:SIDE, b * SIDE : (b + 1) * SIDE]
            imag = coarse[SIDE:, b * SIDE : (b + 1) * SIDE]
            rows = pl.ds(b * SIDE, SIDE)
            rows_high[rows, :SIDE], rows_low[rows, :SIDE] = split(real * cos_turn + imag * sin_turn)
            rows_high[rows, SIDE:], rows_low[rows, SIDE:] = split(imag * cos_turn - real * sin_turn)

    def along_rows(table, count):
        rows = pl.ds(0, count * SIDE)
        return (
            dot(rows_high[rows, :], table[0])
            + dot(rows_low[rows, :], table[0])
            + dot(rows_high[rows, :], table[1])
        )

    def exact_columns(land):
        columns = jnp.concatenate([land[b].astype(BF16) for b in range(4)], axis=1)
        return dot(first[:, : 2 * SIDE], jnp.concatenate([columns, columns], axis=0))

    def inverse(products, count):
        for b in range(count):
            real, imag = products[b]
            rows = pl.ds(b * SIDE, SIDE)
            rows_high[rows, :SIDE], rows_low[rows, :SIDE] = split(real)
            rows_high[rows, SIDE:], rows_low[rows, SIDE:] = split(imag)
        lines = along_rows(third, count)
        for b in range(count):
            real = lines[b * SIDE : (b + 1) * SIDE, :SIDE]
            imag = lines[b * SIDE : (b + 1) * SIDE, SIDE:]
            where = pl.ds(b * SIDE, SIDE)
            columns_high[:SIDE, where], columns_low[:SIDE, where] = split(real * cos_turn - imag * sin_turn)
            columns_high[SIDE:, where], columns_low[SIDE:, where] = split(real * sin_turn + imag * cos_turn)
        where = pl.ds(0, count * SIDE)
        return (
            dot(fourth[0], columns_high[:, where])
            + dot(fourth[0], columns_low[:, where])
            + dot(fourth[1], columns_high[:, where])
        )

    def times_conjugate(left, right):
        return (
            left[0] * right[0] + left[1] * right[1],
            left[1] * right[0] - left[0] * right[1],
        )

    def spectrum(b):
        rows = pl.ds(b * SIDE, SIDE)
        return spectra[rows, :SIDE], spectra[rows, SIDE:]

    all_taps.wait()
    taps_high, taps_low = split(land_taps[...])
    coarse[:, 4 * SIDE :] = dot(first[...], jnp.concatenate([taps_high, taps_high, taps_low], axis=0))
    all_grad.wait()
    coarse[:, : 4 * SIDE] = exact_columns(land_grad)
    turn_forward(5)
    spectra[...] = along_rows(second, 5)
    filter_spectrum = spectrum(4)
    values = inverse([times_conjugate(spectrum(b), filter_spectrum) for b in range(4)], 4)
    for b in range(4):
        send_input[b] = values[:, b * SIDE : (b + 1) * SIDE]
    send_all(
        lambda x, s: send_input.at[pl.ds(2 * x, 2), pl.ds(2 * s, 2), :],
        land_input.at[:, pl.ds(2 * me, 2), :],
        INPUT,
    )
    for b in range(2):
        land_input[b, pl.ds(2 * me, 2), :] = send_input[2 * x_low + b, pl.ds(2 * seq, 2), :]

    all_signal.wait()
    coarse[:, : 4 * SIDE] = exact_columns(land_signal)
    turn_forward(4)
    signal_spectra = along_rows(second, 4)
    total_real, total_imag = 0.0, 0.0
    for b in range(4):
        lines = signal_spectra[b * SIDE : (b + 1) * SIDE]
        real, imag = times_conjugate(spectrum(b), (lines[:, :SIDE], lines[:, SIDE:]))
        total_real, total_imag = total_real + real, total_imag + imag
    send_filter[...] = inverse([(total_real, total_imag)], 1)
    send_all(
        lambda x, s: send_filter.at[pl.ds(2 * s, 2), :], land_filter.at[pl.ds(2 * me, 2), :], FILTER
    )
    land_filter[pl.ds(2 * me, 2), :] = send_filter[pl.ds(2 * seq, 2), :]

    all_input = copy(land_input.at[:, pl.ds(0, 254), :], land_input.at[:, pl.ds(0, 254), :], INPUT, partner)
    all_input.wait()
    swap_input = copy(land_input.at[1 - core], pair_input, SWAP_INPUT, partner)
    swap_input.start()

    def finish_input(block_of, lanes):
        for half in range(2):
            rows = pl.ds(half * SIDE, SIDE)
            skip = gain[:, pl.ds(lanes, SIDE)] * grad[rows, pl.ds(lanes, SIDE)].astype(F32)
            out_input[rows, pl.ds(lanes, SIDE)] = (block_of(half).T + skip).astype(BF16)

    finish_input(lambda half: land_input[core, pl.ds(half, SIDE, stride=2), :], own)
    swap_input.wait()
    finish_input(lambda half: pair_input[pl.ds(half, SIDE, stride=2), :], other)

    all_filter = copy(land_filter.at[pl.ds(0, 254)], land_filter.at[pl.ds(0, 254)], FILTER, partner)
    all_filter.wait()
    swap_filter = copy(land_filter, pair_filter, SWAP_FILTER, partner)
    swap_filter.start()
    for half in range(2):
        out_filter[pl.ds(half * SIDE, SIDE), pl.ds(own, SIDE)] = land_filter[pl.ds(half, SIDE, stride=2), :].T
    swap_filter.wait()
    for half in range(2):
        out_filter[pl.ds(half * SIDE, SIDE), pl.ds(other, SIDE)] = pair_filter[pl.ds(half, SIDE, stride=2), :].T


def put_out(input_near, filter_near, input_far, filter_far, sems):
    copies = [
        pltpu.make_async_copy(filter_near, filter_far, sems.at[0]),
        pltpu.make_async_copy(input_near, input_far, sems.at[1]),
    ]
    for copy in copies:
        copy.start()
    for copy in copies:
        copy.wait()


def shards(signal, grad_out, filter_taps, skip_gain):
    vmem = pl.BlockSpec(memory_space=pltpu.VMEM)
    held = tables()
    rows = lambda *shape: pltpu.VMEM((*shape, SIDE), F32)
    input_grad, filter_grad = pl.pallas_call(
        body,
        out_shape=(
            pltpu.VMEM((2 * SIDE, 2 * SIDE), BF16),
            pltpu.VMEM((2 * SIDE, 2 * SIDE), F32),
        ),
        in_specs=[pl.BlockSpec(memory_space=pl.ANY)] * 9,
        out_specs=(vmem, vmem),
        scratch_shapes=[
            pltpu.VMEM((2 * SIDE, 2 * SIDE), BF16),
            pltpu.VMEM((2 * SIDE, 2 * SIDE), BF16),
            rows(SIDE),
            pltpu.VMEM((1, 2 * SIDE), F32),
            *(pltpu.VMEM(table.shape, table.dtype) for table in held),
            rows(SIDE), rows(2, 2 * SIDE), rows(2, 2 * SIDE), rows(2 * SIDE), rows(2 * SIDE),
            rows(SIDE), rows(4, SIDE), rows(4, SIDE),
            rows(4, SIDE), rows(SIDE), rows(2, 2 * SIDE), rows(2 * SIDE), rows(2 * SIDE), rows(2 * SIDE),
            pltpu.VMEM((2 * SIDE, 5 * SIDE), F32),
            pltpu.VMEM((5 * SIDE, 2 * SIDE), BF16),
            pltpu.VMEM((5 * SIDE, 2 * SIDE), BF16),
            pltpu.VMEM((5 * SIDE, 2 * SIDE), F32),
            pltpu.VMEM((2 * SIDE, 4 * SIDE), BF16),
            pltpu.VMEM((2 * SIDE, 4 * SIDE), BF16),
            pltpu.SemaphoreType.DMA((9,)),
            pltpu.SemaphoreType.DMA((9,)),
            pltpu.SemaphoreType.DMA((9,)),
        ],
        compiler_params=pltpu.CompilerParams(collective_id=0, has_side_effects=True),
    )(signal[0], grad_out[0], filter_taps, skip_gain[None, :], *held)
    place = pl.BlockSpec(memory_space=pl.ANY)
    input_grad, filter_grad = pl.pallas_call(
        put_out,
        out_shape=(
            jax.ShapeDtypeStruct((2 * SIDE, 2 * SIDE), BF16),
            jax.ShapeDtypeStruct((2 * SIDE, 2 * SIDE), F32),
        ),
        in_specs=[vmem] * 2,
        out_specs=(place, place),
        scratch_shapes=[pltpu.SemaphoreType.DMA((2,))],
    )(*(pltpu.with_memory_space_constraint(x, pltpu.VMEM) for x in (input_grad, filter_grad)))
    return input_grad[None], filter_grad


def solution(mesh):
    return jax.shard_map(
        shards,
        mesh=mesh,
        in_specs=(P("batch", "seq", None), P("batch", "seq", None), P("seq", None), P()),
        out_specs=(P("batch", "seq", None), P("seq", None)),
        check_vma=False,
    )
```

```python
import ml_dtypes
import numpy as np
import jax
import jax.numpy as jnp
from jax import lax
from jax.experimental import pallas as pl
from jax.experimental.pallas import tpu as pltpu
from jax.sharding import PartitionSpec as P


F32 = jnp.float32
BF16 = jnp.bfloat16
SIDE = 128
LEN = SIDE * SIDE
LOGICAL = pl.DeviceIdType.LOGICAL
TAPS, GRAD, SIGNAL, INPUT, FILTER, SWAP_GRAD, SWAP_SIGNAL, SWAP_INPUT, SWAP_FILTER = range(9)


ORDER = sorted(
    [(dx, dy, dz) for dz in range(8) for dy in range(4) for dx in range(4) if dx + dy + dz],
    key=lambda d: (-sum(min(step, size - step) for step, size in zip(d, (4, 4, 8))), min(d[2], 8 - d[2])),
)


def split_table(table):
    high = table.astype(np.float32).astype(ml_dtypes.bfloat16)
    low = (table - high.astype(np.float64)).astype(np.float32).astype(ml_dtypes.bfloat16)
    return high, low


def tables():
    index = np.arange(SIDE)
    angle = 2 * np.pi * (np.outer(4 * index + 1, index) % (4 * SIDE)) / (4.0 * SIDE)
    high, low = split_table(np.concatenate([np.cos(angle), -np.sin(angle)], axis=0))
    first = np.concatenate([high, low, high], axis=1)
    fine = 2 * np.pi * (np.outer(index, index) % SIDE) / float(SIDE)
    cos_fine, sin_fine = np.cos(fine), np.sin(fine)
    second = np.stack(split_table(np.block([[cos_fine, -sin_fine], [sin_fine, cos_fine]])))
    third = np.stack(split_table(np.block([[cos_fine, sin_fine], [-sin_fine, cos_fine]])))
    fourth = np.stack(split_table(np.concatenate([np.cos(angle.T), -np.sin(angle.T)], axis=1) / LEN))
    turn = 2 * np.pi * np.outer(4 * index + 1, index) / (4.0 * LEN)
    turns = np.stack([np.cos(turn), np.sin(turn)]).astype(np.float32)
    return tuple(jnp.asarray(table) for table in (first, second, third, fourth, turns))


def split(value):
    high = value.astype(BF16)
    return high, (value - high.astype(F32)).astype(BF16)


def dot(left, right):
    return jnp.dot(left, right, preferred_element_type=F32)


def body(
    signal_far, grad_far, taps_far, gain_far, *rest
):
    (
        tables_far, (out_input, out_filter), (signal, grad, taps, gain), held_tables, rest
    ) = rest[:5], rest[5:7], rest[7:11], rest[11:16], rest[16:]
    run(signal_far, grad_far, taps_far, gain_far, tables_far, out_input, out_filter,
        signal, grad, taps, gain, *held_tables, held_tables, *rest)


def run(
    signal_far, grad_far, taps_far, gain_far, tables_far,
    out_input, out_filter,
    signal, grad, taps, gain, first, second, third, fourth, turns, held_tables,
    send_taps, send_grad, send_signal, stage_grad, stage_signal, land_taps, land_grad, land_signal,
    send_input, send_filter, land_input, land_filter, pair_input, pair_filter,
    coarse, rows_high, rows_low, spectra, columns_high, columns_low,
    sends, recvs, loads,
):
    batch = lax.axis_index("batch")
    seq = lax.axis_index("seq")
    core = batch % 2
    x_low = batch // 2
    x_pos = 2 * ((seq // 8) % 2) + x_low
    y_pos = seq // 16
    z_pos = seq % 8
    me = x_low * 64 + seq
    partner = (batch + 1 - 2 * core) * 64 + seq
    own = pl.multiple_of(core * SIDE, SIDE)
    other = pl.multiple_of((1 - core) * SIDE, SIDE)

    sign = 1 - 2 * core
    z_places = [(z_pos + sign * dz + 8) % 8 for dz in range(8)]
    y_places = [((y_pos + dy) % 4) * 16 for dy in range(4)]
    x_places = []
    for dx in range(4):
        x_to = (x_pos + dx) % 4
        high = (x_to // 2) * 8
        x_places.append((x_to % 2, high, high + (x_to % 2) * 128 + core * 64))

    def each_peer(act):
        for dx, dy, dz in ORDER:
            place = y_places[dy] + z_places[dz]
            x, high, device = x_places[dx]
            act(x, place + high, place + device)

    def copy(source, landing, slot, device):
        return pltpu.make_async_remote_copy(
            src_ref=source, dst_ref=landing, send_sem=sends.at[slot], recv_sem=recvs.at[slot],
            device_id=device, device_id_type=LOGICAL,
        )

    def send_all(source_of, landing, slot):
        each_peer(lambda x, s, device: copy(source_of(x, s), landing, slot, device).start())

    x_rows = pl.ds(pl.multiple_of(x_low * SIDE, SIDE), SIDE)
    load_grad, load_signal, load_taps, load_gain, *load_tables = [
        pltpu.make_async_copy(far, near, loads.at[slot])
        for slot, (far, near) in enumerate(
            [
                (grad_far, grad), (signal_far, signal), (taps_far.at[x_rows, pl.ds(own, SIDE)], taps),
                (gain_far, gain), *zip(tables_far, held_tables),
            ]
        )
    ]
    for load in (load_grad, load_signal, load_taps, load_gain, *load_tables):
        load.start()

    barrier = pltpu.get_barrier_semaphore()
    each_peer(
        lambda x, s, device: pl.semaphore_signal(
            barrier, inc=1, device_id=device, device_id_type=LOGICAL
        )
    )
    pl.semaphore_signal(barrier, inc=1, device_id=partner, device_id_type=LOGICAL)

    for load, array, stage, send in (
        (load_grad, grad, stage_grad, send_grad), (load_signal, signal, stage_signal, send_signal)
    ):
        load.wait()
        for half in range(2):
            rows = pl.ds(half * SIDE, SIDE)
            spread = pl.ds(half, SIDE, stride=2)
            stage[spread, :] = array[rows, pl.ds(other, SIDE)].astype(F32).T
            send[core, spread, :] = array[rows, pl.ds(own, SIDE)].astype(F32).T
    load_taps.wait()
    send_taps[...] = taps[...].T
    pl.semaphore_wait(barrier, 128)

    swap_grad = copy(stage_grad, send_grad.at[core], SWAP_GRAD, partner)
    swap_signal = copy(stage_signal, send_signal.at[core], SWAP_SIGNAL, partner)
    swap_grad.start()

    taps_at = land_taps.at[pl.ds(2 * seq + x_low, 1)]
    send_all(lambda x, s: send_taps.at[pl.ds(64 * x + s, 1)], taps_at, TAPS)
    land_taps[pl.ds(2 * seq + x_low, 1), :] = send_taps[pl.ds(me, 1), :]

    for swap, send, land, slot in (
        (swap_grad, send_grad, land_grad, GRAD),
        (swap_signal, send_signal, land_signal, SIGNAL),
    ):
        swap.wait()
        if slot == GRAD:
            swap_signal.start()
        send_all(
            lambda x, s, send=send: send.at[:, pl.ds(128 * x + 2 * s, 2), :],
            land.at[pl.ds(2 * x_low, 2), pl.ds(2 * seq, 2), :],
            slot,
        )
        for b in range(2):
            land[2 * x_low + b, pl.ds(2 * seq, 2), :] = send[b, pl.ds(2 * me, 2), :]

    all_taps = copy(land_taps.at[pl.ds(0, 127)], land_taps.at[pl.ds(0, 127)], TAPS, partner)
    all_grad, all_signal = (
        copy(land.at[:, pl.ds(0, 127), :], land.at[:, pl.ds(0, 127), :], slot, partner)
        for land, slot in ((land_grad, GRAD), (land_signal, SIGNAL))
    )

    for load in (load_gain, *load_tables):
        load.wait()
    cos_turn, sin_turn = turns[0], turns[1]

    def turn_forward(count):
        for b in range(count):
            real = coarse[:SIDE, b * SIDE : (b + 1) * SIDE]
            imag = coarse[SIDE:, b * SIDE : (b + 1) * SIDE]
            rows = pl.ds(b * SIDE, SIDE)
            rows_high[rows, :SIDE], rows_low[rows, :SIDE] = split(real * cos_turn + imag * sin_turn)
            rows_high[rows, SIDE:], rows_low[rows, SIDE:] = split(imag * cos_turn - real * sin_turn)

    def along_rows(table, count):
        rows = pl.ds(0, count * SIDE)
        return (
            dot(rows_high[rows, :], table[0])
            + dot(rows_low[rows, :], table[0])
            + dot(rows_high[rows, :], table[1])
        )

    def exact_columns(land):
        columns = jnp.concatenate([land[b].astype(BF16) for b in range(4)], axis=1)
        return dot(first[:, : 2 * SIDE], jnp.concatenate([columns, columns], axis=0))

    def inverse(products, count):
        for b in range(count):
            real, imag = products[b]
            rows = pl.ds(b * SIDE, SIDE)
            rows_high[rows, :SIDE], rows_low[rows, :SIDE] = split(real)
            rows_high[rows, SIDE:], rows_low[rows, SIDE:] = split(imag)
        lines = along_rows(third, count)
        for b in range(count):
            real = lines[b * SIDE : (b + 1) * SIDE, :SIDE]
            imag = lines[b * SIDE : (b + 1) * SIDE, SIDE:]
            where = pl.ds(b * SIDE, SIDE)
            columns_high[:SIDE, where], columns_low[:SIDE, where] = split(real * cos_turn - imag * sin_turn)
            columns_high[SIDE:, where], columns_low[SIDE:, where] = split(real * sin_turn + imag * cos_turn)
        where = pl.ds(0, count * SIDE)
        return (
            dot(fourth[0], columns_high[:, where])
            + dot(fourth[0], columns_low[:, where])
            + dot(fourth[1], columns_high[:, where])
        )

    def times_conjugate(left, right):
        return (
            left[0] * right[0] + left[1] * right[1],
            left[1] * right[0] - left[0] * right[1],
        )

    def spectrum(b):
        rows = pl.ds(b * SIDE, SIDE)
        return spectra[rows, :SIDE], spectra[rows, SIDE:]

    all_taps.wait()
    taps_high, taps_low = split(land_taps[...])
    coarse[:, 4 * SIDE :] = dot(first[...], jnp.concatenate([taps_high, taps_high, taps_low], axis=0))
    all_grad.wait()
    coarse[:, : 4 * SIDE] = exact_columns(land_grad)
    turn_forward(5)
    spectra[...] = along_rows(second, 5)
    filter_spectrum = spectrum(4)
    values = inverse([times_conjugate(spectrum(b), filter_spectrum) for b in range(4)], 4)
    for b in range(4):
        send_input[b] = values[:, b * SIDE : (b + 1) * SIDE]
    send_all(
        lambda x, s: send_input.at[pl.ds(2 * x, 2), pl.ds(2 * s, 2), :],
        land_input.at[:, pl.ds(2 * me, 2), :],
        INPUT,
    )
    for b in range(2):
        land_input[b, pl.ds(2 * me, 2), :] = send_input[2 * x_low + b, pl.ds(2 * seq, 2), :]

    all_signal.wait()
    coarse[:, : 4 * SIDE] = exact_columns(land_signal)
    turn_forward(4)
    signal_spectra = along_rows(second, 4)
    total_real, total_imag = 0.0, 0.0
    for b in range(4):
        lines = signal_spectra[b * SIDE : (b + 1) * SIDE]
        real, imag = times_conjugate(spectrum(b), (lines[:, :SIDE], lines[:, SIDE:]))
        total_real, total_imag = total_real + real, total_imag + imag
    send_filter[...] = inverse([(total_real, total_imag)], 1)
    send_all(
        lambda x, s: send_filter.at[pl.ds(2 * s, 2), :], land_filter.at[pl.ds(2 * me, 2), :], FILTER
    )
    land_filter[pl.ds(2 * me, 2), :] = send_filter[pl.ds(2 * seq, 2), :]

    all_input = copy(land_input.at[:, pl.ds(0, 254), :], land_input.at[:, pl.ds(0, 254), :], INPUT, partner)
    all_input.wait()
    swap_input = copy(land_input.at[1 - core], pair_input, SWAP_INPUT, partner)
    swap_input.start()

    def finish_input(block_of, lanes):
        for half in range(2):
            rows = pl.ds(half * SIDE, SIDE)
            skip = gain[:, pl.ds(lanes, SIDE)] * grad[rows, pl.ds(lanes, SIDE)].astype(F32)
            out_input[rows, pl.ds(lanes, SIDE)] = (block_of(half).T + skip).astype(BF16)

    finish_input(lambda half: land_input[core, pl.ds(half, SIDE, stride=2), :], own)
    swap_input.wait()
    finish_input(lambda half: pair_input[pl.ds(half, SIDE, stride=2), :], other)

    all_filter = copy(land_filter.at[pl.ds(0, 254)], land_filter.at[pl.ds(0, 254)], FILTER, partner)
    all_filter.wait()
    swap_filter = copy(land_filter, pair_filter, SWAP_FILTER, partner)
    swap_filter.start()
    for half in range(2):
        out_filter[1, pl.ds(half * SIDE, SIDE), :] = land_filter[pl.ds(half, SIDE, stride=2), :].T
    swap_filter.wait()
    out_filter[0] = pair_filter[...]


def put_out(input_near, filter_near, input_far, filter_far, turned, sems):
    core = lax.axis_index("batch") % 2
    own = filter_far.at[:, pl.ds(pl.multiple_of(core * SIDE, SIDE), SIDE)]
    other = filter_far.at[:, pl.ds(pl.multiple_of((1 - core) * SIDE, SIDE), SIDE)]
    copies = [
        pltpu.make_async_copy(filter_near.at[1], own, sems.at[0]),
        pltpu.make_async_copy(input_near, input_far, sems.at[1]),
        pltpu.make_async_copy(turned, other, sems.at[2]),
    ]
    copies[0].start()
    copies[1].start()
    for half in range(2):
        turned[pl.ds(half * SIDE, SIDE), :] = filter_near[0, pl.ds(half, SIDE, stride=2), :].T
    copies[2].start()
    for copy in copies:
        copy.wait()


def shards(signal, grad_out, filter_taps, skip_gain):
    vmem = pl.BlockSpec(memory_space=pltpu.VMEM)
    held = tables()
    rows = lambda *shape: pltpu.VMEM((*shape, SIDE), F32)
    input_grad, filter_grad = pl.pallas_call(
        body,
        out_shape=(
            pltpu.VMEM((2 * SIDE, 2 * SIDE), BF16),
            rows(2, 2 * SIDE),
        ),
        in_specs=[pl.BlockSpec(memory_space=pl.ANY)] * 9,
        out_specs=(vmem, vmem),
        scratch_shapes=[
            pltpu.VMEM((2 * SIDE, 2 * SIDE), BF16),
            pltpu.VMEM((2 * SIDE, 2 * SIDE), BF16),
            rows(SIDE),
            pltpu.VMEM((1, 2 * SIDE), F32),
            *(pltpu.VMEM(table.shape, table.dtype) for table in held),
            rows(SIDE), rows(2, 2 * SIDE), rows(2, 2 * SIDE), rows(2 * SIDE), rows(2 * SIDE),
            rows(SIDE), rows(4, SIDE), rows(4, SIDE),
            rows(4, SIDE), rows(SIDE), rows(2, 2 * SIDE), rows(2 * SIDE), rows(2 * SIDE), rows(2 * SIDE),
            pltpu.VMEM((2 * SIDE, 5 * SIDE), F32),
            pltpu.VMEM((5 * SIDE, 2 * SIDE), BF16),
            pltpu.VMEM((5 * SIDE, 2 * SIDE), BF16),
            pltpu.VMEM((5 * SIDE, 2 * SIDE), F32),
            pltpu.VMEM((2 * SIDE, 4 * SIDE), BF16),
            pltpu.VMEM((2 * SIDE, 4 * SIDE), BF16),
            pltpu.SemaphoreType.DMA((9,)),
            pltpu.SemaphoreType.DMA((9,)),
            pltpu.SemaphoreType.DMA((9,)),
        ],
        compiler_params=pltpu.CompilerParams(collective_id=0, has_side_effects=True),
    )(signal[0], grad_out[0], filter_taps, skip_gain[None, :], *held)
    place = pl.BlockSpec(memory_space=pl.ANY)
    input_grad, filter_grad = pl.pallas_call(
        put_out,
        out_shape=(
            jax.ShapeDtypeStruct((2 * SIDE, 2 * SIDE), BF16),
            jax.ShapeDtypeStruct((2 * SIDE, 2 * SIDE), F32),
        ),
        in_specs=[vmem] * 2,
        out_specs=(place, place),
        scratch_shapes=[rows(2 * SIDE), pltpu.SemaphoreType.DMA((3,))],
    )(*(pltpu.with_memory_space_constraint(x, pltpu.VMEM) for x in (input_grad, filter_grad)))
    return input_grad[None], filter_grad


def solution(mesh):
    return jax.shard_map(
        shards,
        mesh=mesh,
        in_specs=(P("batch", "seq", None), P("batch", "seq", None), P("seq", None), P()),
        out_specs=(P("batch", "seq", None), P("seq", None)),
        check_vma=False,
    )
```
